128 devices in a mesh: row: 8 (over z, x_hi), col: 16 (over y, x_lo, core).
Axes of the slice: x: 4 (x_hi: 2, x_lo: 2; x = x_hi * 2 + x_lo), y: 4, z: 4, core: 2. Of those that a mesh axis runs over, the one named last changes fastest.
Arguments:
- diag_blocks: float32 [16, 32, 512, 512], P('row', 'col'), may hold values from -4 to 16, as said below
- horizontal: bfloat16 [16, 32, 512, 512], P('row', 'col'), may hold values from -0.125 to 0.125
- vertical: bfloat16 [16, 32, 512, 512], P('row', 'col'), may hold values from -0.125 to 0.125
Outputs:
- red_factor: float32 [16, 16, 512, 512], P('row', 'col')
- black_schur: float32 [16, 16, 512, 512], P('row', 'col')
- black_links: bfloat16 [16, 16, 4, 512, 512], P('row', 'col')
The draws below stay inside these ranges and needn't reach their ends.
Inputs may be any that keep to these rules, and one draw needn't show every extreme that they name: `diag_blocks`: every block is symmetric and its eigenvalues are at least 1.
All inputs are finite; a program needn't handle non-finite values.
Results may differ from the reference program's by a relative error of at most 0.0054.
Values may be sent and summed in bfloat16 or wider, within the bound.
A program may use at most 128 MiB of HBM per device.

```python
import math
import jax
import jax.numpy as jnp
from jax import lax

BLOCK = 512
GRID_ROWS = 16
GRID_COLS = 32


def draw_diag_blocks(key, part):
    first_key = jax.random.fold_in(key, 11)
    second_key = jax.random.fold_in(key, 12)
    factor = jax.random.normal(first_key, (GRID_ROWS, GRID_COLS, BLOCK, BLOCK), jnp.float32)
    levels = jnp.exp(jax.random.uniform(second_key, (GRID_ROWS, GRID_COLS, BLOCK), jnp.float32, 0.0, math.log(4.0)))
    strength = 2.0
    gram = jnp.einsum('rcik,rcjk->rcij', factor, factor, precision=lax.Precision.HIGHEST) * (strength / BLOCK)
    return gram + levels[..., None] * jnp.eye(BLOCK, dtype=jnp.float32)


def block_levels(rng, dims, split, smallest, top_value):
    def one(position, parts):
        heights = jax.random.uniform(jax.random.fold_in(jax.random.fold_in(rng, 6), position), (parts,), jnp.float32, smallest / len(split), top_value / len(split))
        return jnp.repeat(jnp.exp(heights), dims[position] // parts).reshape((-1,) + (1,) * (len(dims) - position - 1))

    level = one(*split[0])
    for cut in split[1:]:
        level = level * one(*cut)
    return level


def gaussian(rng, shape, width, most, pieces=(), kind=jnp.bfloat16):
    factor_of = block_levels(rng, shape, pieces, -0.22, 0.18) if pieces else 1.0
    drawn = jax.random.normal(rng, shape, jnp.float32) * width * factor_of
    return jnp.minimum(jnp.maximum(drawn, -most), most).astype(kind)


def setup_inputs(seed: int = 0) -> dict:
    keys = jax.random.split(jax.random.key(seed), 4)
    diag_blocks = draw_diag_blocks(jax.random.fold_in(keys[3], 71), 0)
    horizontal = gaussian(keys[1], (GRID_ROWS, GRID_COLS, BLOCK, BLOCK), (4 * BLOCK) ** -0.5, 0.125, ((0, 8), (1, 16)))
    vertical = gaussian(keys[2], (GRID_ROWS, GRID_COLS, BLOCK, BLOCK), (4 * BLOCK) ** -0.5, 0.125, ((0, 8), (1, 16)))
    return dict(diag_blocks=diag_blocks, horizontal=horizontal, vertical=vertical)


def select_colour(blocks, parity):
    grid_rows = blocks.shape[0]
    grid_columns = blocks.shape[1]
    trailing = blocks.shape[2:]
    paired = blocks.reshape((grid_rows // 2, 2, grid_columns // 2, 2) + trailing)
    joined = jnp.stack([paired[:, 0, :, parity], paired[:, 1, :, 1 - parity]], 1)
    return joined.reshape((grid_rows, grid_columns // 2) + trailing)

def combine_rows(even_rows, odd_rows):
    joined = jnp.stack([even_rows, odd_rows], 1)
    return joined.reshape((2 * even_rows.shape[0],) + even_rows.shape[1:])

def transposed(blocks):
    return jnp.swapaxes(blocks, -1, -2)

def gram_term(former, latter):
    return jnp.einsum('mka,mkb->mab', former.astype(jnp.float32), latter.astype(jnp.float32), precision=lax.Precision.HIGHEST)

def solve_red(packed):
    factor = jnp.linalg.cholesky(packed[0])
    results = [jax.scipy.linalg.solve_triangular(factor, coupling, lower=True) for coupling in packed[1:]]
    return (factor, jnp.stack(results, 1).astype(jnp.bfloat16))

def black_row(packed):
    diag_black, above, below, left_red, right_red = packed
    update = gram_term(above[:, 3], above[:, 3]) + gram_term(below[:, 1], below[:, 1])
    update = update + gram_term(left_red[:, 2], left_red[:, 2]) + gram_term(right_red[:, 0], right_red[:, 0])
    schur_part = diag_black - update
    east_link = -gram_term(right_red[:, 0], right_red[:, 2])
    south_link = -gram_term(below[:, 1], below[:, 3])
    southeast = -(gram_term(right_red[:, 0], right_red[:, 3]) + gram_term(below[:, 1], below[:, 2]))
    southwest = -(gram_term(left_red[:, 2], left_red[:, 3]) + gram_term(below[:, 1], below[:, 0]))
    links = jnp.stack([east_link, south_link, southeast, southwest], 1).astype(jnp.bfloat16)
    return (schur_part, links)

def reference(diag_blocks, horizontal, vertical):
    left_links = jnp.roll(horizontal, 1, axis=1)
    upper_links = jnp.roll(vertical, 1, axis=0)
    couplings = (transposed(select_colour(left_links, 0)).astype(jnp.float32), transposed(select_colour(upper_links, 0)).astype(jnp.float32), select_colour(horizontal, 0).astype(jnp.float32), select_colour(vertical, 0).astype(jnp.float32))
    red_factor, solved = lax.map(solve_red, (select_colour(diag_blocks, 0),) + couplings)
    above = jnp.roll(solved, 1, axis=0)
    below = jnp.roll(solved, -1, axis=0)
    previous = jnp.roll(solved, 1, axis=1)
    following = jnp.roll(solved, -1, axis=1)
    left_red = combine_rows(solved[0::2], previous[1::2])
    right_red = combine_rows(following[0::2], solved[1::2])
    black_schur, black_links = lax.map(black_row, (select_colour(diag_blocks, 1), above, below, left_red, right_red))
    return (red_factor, black_schur, black_links)
```

```python
import functools

import jax
import jax.numpy as jnp
from jax import lax
from jax.experimental import pallas as pl
from jax.experimental.pallas import tpu as pltpu
from jax.sharding import PartitionSpec as P

N = 512
NB = 128
SB = 16
F32 = jnp.float32
BF16 = jnp.bfloat16


def dot(a, b, ca=1, cb=0):
    return lax.dot_general(a, b, (((ca,), (cb,)), ((), ())), preferred_element_type=F32)


def split(x):
    hi = x.astype(BF16)
    return hi, (x - hi.astype(F32)).astype(BF16)


def dot3(a, b, cb=0):
    ah, al = a
    bh, bl = b
    if cb == 1:
        return dot(ah, bh, 1, 1) + dot(al, bh, 1, 1) + dot(ah, bl, 1, 1)
    return dot(jnp.concatenate([ah, al], 1), jnp.concatenate([bh, bh], 0)) + dot(ah, bl)


def rows8(x, k):
    return jnp.broadcast_to(x[k : k + 1, :], (8, NB))


def eliminate(s, x_ref, p_ref):
    k0 = SB * s
    row = lax.broadcasted_iota(jnp.int32, (8, NB), 0)
    xs = [[x_ref[k0 + 8 * h : k0 + 8 * h + 8, NB * w : NB * w + NB] for h in range(2)] for w in range(2)]
    cols = [
        [jnp.broadcast_to(xs[0][h][:, k0 + c : k0 + c + 1], (8, NB)) for h in range(2)]
        for c in range(SB)
    ]
    pivots = [jnp.ones((8, NB), F32) for _ in range(2)]
    saved = [[xs[w][h] for h in range(2)] for w in range(2)]
    for k in range(SB):
        kh, kr = divmod(k, 8)
        is_k = row == kr
        pivot = rows8(cols[k][kh], kr)
        inverse = 1.0 / pivot
        mult = [cols[k][h] * inverse for h in range(2)]
        mult[kh] = jnp.where(is_k, 0.0, mult[kh])
        for c in range(k + 1, SB):
            head = rows8(cols[c][kh], kr)
            cols[c] = [cols[c][h] - mult[h] * head for h in range(2)]
        pivots[kh] = jnp.where(is_k, pivot, pivots[kh])
        for w in range(2):
            saved[w][kh] = jnp.where(is_k, xs[w][kh], saved[w][kh])
            head = rows8(xs[w][kh], kr)
            xs[w] = [xs[w][h] - mult[h] * head for h in range(2)]
    for h in range(2):
        scale = lax.rsqrt(pivots[h])
        for w in range(2):
            p_ref[k0 + 8 * h : k0 + 8 * h + 8, NB * w : NB * w + NB] = saved[w][h] * scale
    below = NB - k0 - SB
    if below:
        z = jnp.concatenate(
            [jnp.concatenate([xs[w][h] / pivots[h] for w in range(2)], 1) for h in range(2)], 0
        )
        zh, zl = split(z)

        def pad(v):
            parts = [v]
            if k0:
                parts.insert(0, jnp.zeros((k0, 2 * NB), BF16))
            parts.append(jnp.zeros((below, 2 * NB), BF16))
            return jnp.concatenate(parts, 0)

        a = split(x_ref[k0 + SB : NB, 0:NB])
        x_ref[k0 + SB : NB, :] = x_ref[k0 + SB : NB, :] - dot3(a, (pad(zh), pad(zl)))


def factor_all(g_refs, x_refs, p_refs, w_refs, l_refs, inv_refs):
    r_i = lax.broadcasted_iota(jnp.int32, (NB, NB), 0)
    c_i = lax.broadcasted_iota(jnp.int32, (NB, NB), 1)
    wide = lax.broadcasted_iota(jnp.int32, (NB, N), 1)
    for l_ref in l_refs:
        l_ref[...] = jnp.zeros_like(l_ref)

    def outer(o, carry):
        base = pl.multiple_of(o * NB, NB)
        here = pl.ds(base, NB)
        for g_ref, x_ref in zip(g_refs, x_refs):
            x_ref[:, 0:NB] = g_ref[here, here]
            x_ref[:, NB : 2 * NB] = jnp.where(r_i == c_i, 1.0, 0.0)
        for s in range(NB // SB):
            for x_ref, p_ref in zip(x_refs, p_refs):
                eliminate(s, x_ref, p_ref)
        for g_ref, p_ref, w_ref, l_ref, inv_ref in zip(g_refs, p_refs, w_refs, l_refs, inv_refs):
            upper = p_ref[:, 0:NB]
            l_ref[here, here] = jnp.where(r_i >= c_i, upper.T, 0.0)
            inverse = p_ref[:, NB : 2 * NB]
            w_ref[...] = dot3(split(inverse), split(g_ref[here, :]))
            w_ref[:, here] = inverse
            inv_ref[here, :] = jnp.where(wide < base + NB, w_ref[...], 0.0).astype(BF16)
        for p in range(1, N // NB):
            rows = slice(p * NB, (p + 1) * NB)

            @pl.when(p > o)
            def _():
                for g_ref, p_ref, w_ref, l_ref in zip(g_refs, p_refs, w_refs, l_refs):
                    lower = dot3(split(g_ref[rows, here]), split(p_ref[:, NB : 2 * NB]), 1)
                    l_ref[rows, here] = lower
                    g_ref[rows, here] = jnp.zeros((NB, NB), F32)
                    g_ref[rows, :] = g_ref[rows, :] - dot3(split(lower), split(w_ref[...]))

        return carry

    lax.fori_loop(0, N // NB, outer, 0)


def solve_t(inv_ref, c_ref, out_ref):
    h = N // 2
    out_ref[:, 0:h] = dot(c_ref[:, 0:h], inv_ref[0:h, 0:h], 1, 1).astype(BF16)
    out_ref[:, h:N] = dot(c_ref[...], inv_ref[h:N, :], 1, 1).astype(BF16)


def solve_n(inv_ref, c_ref, out_ref):
    h = N // 2
    out_ref[0:h, :] = dot(inv_ref[0:h, 0:h], c_ref[0:h, :]).astype(BF16)
    out_ref[h:N, :] = dot(inv_ref[h:N, :], c_ref[...]).astype(BF16)


def packed_blocks():
    return [(r, c) for r in range(N // NB) for c in range(r + 1)]


def put_packed(dst_ref, first, value):
    for b, (r, c) in enumerate(packed_blocks()):
        dst_ref[first + b] = value[r * NB : (r + 1) * NB, c * NB : (c + 1) * NB].astype(BF16)


def local_kernel(d_ref, h_ref, v_ref, l_out, inv_out, right_out, down_out, schur_out, link_out, se_out,
                 g0, g1, x0, x1, p0, p1, w0, w1, l0, l1, i0, i1, dbuf, hv, hh, y0, y1, y2, y3, z2, z3,
                 sbuf, lbuf, in_sem, out_sem):
    copies = [
        pltpu.make_async_copy(d_ref.at[0, 0], g0, in_sem.at[0]),
        pltpu.make_async_copy(d_ref.at[1, 1], g1, in_sem.at[1]),
        pltpu.make_async_copy(d_ref.at[0, 1], sbuf.at[0], in_sem.at[2]),
        pltpu.make_async_copy(d_ref.at[1, 0], sbuf.at[1], in_sem.at[3]),
        pltpu.make_async_copy(h_ref, hh, in_sem.at[4]),
        pltpu.make_async_copy(v_ref, hv, in_sem.at[5]),
    ]
    for c in copies:
        c.start()
    copies[0].wait()
    copies[1].wait()
    factor_all((g0, g1), (x0, x1), (p0, p1), (w0, w1), (l0, l1), (i0, i1))
    outs = [
        pltpu.make_async_copy(l0, l_out.at[0, 0], out_sem.at[0]),
        pltpu.make_async_copy(l1, l_out.at[1, 0], out_sem.at[1]),
    ]
    for c in outs:
        c.start()
    for c in copies[2:]:
        c.wait()
    for b, (r, c) in enumerate(packed_blocks()):
        inv_out[b] = i0[r * NB : (r + 1) * NB, c * NB : (c + 1) * NB]
    solve_n(i1, hh.at[1, 1], y2)
    solve_n(i1, hv.at[1, 1], y3)
    t2 = y2[...].T
    put_packed(right_out, 0, dot(t2, y2[...]))
    side = dot(t2, y3[...]).astype(BF16)
    for r in range(4):
        for c in range(4):
            right_out[10 + 4 * r + c] = side[r * NB : (r + 1) * NB, c * NB : (c + 1) * NB]
    put_packed(down_out, 0, dot(y3[...].T, y3[...]))
    solve_t(i1, hh.at[1, 0], y0)
    solve_t(i1, hv.at[0, 1], y1)
    solve_n(i0, hh.at[0, 0], z2)
    solve_n(i0, hv.at[0, 0], z3)
    u2 = z2[...].T
    sbuf[0] = sbuf[0] - (dot(u2, z2[...]) + dot(y1[...], y1[...], 1, 1))
    sbuf[1] = sbuf[1] - (dot(z3[...].T, z3[...]) + dot(y0[...], y0[...], 1, 1))
    lbuf[0] = (-dot(y1[...], y3[...])).astype(BF16)
    lbuf[1] = (-(dot(u2, z3[...]) + dot(y1[...], y0[...], 1, 1))).astype(BF16)
    lbuf[2] = (-dot(y0[...], y2[...])).astype(BF16)
    dbuf[0] = dot(y1[...], y2[...])
    dbuf[1] = dot(y0[...], y3[...])
    outs += [
        pltpu.make_async_copy(sbuf.at[0], schur_out.at[0, 0], out_sem.at[2]),
        pltpu.make_async_copy(sbuf.at[1], schur_out.at[1, 0], out_sem.at[3]),
        pltpu.make_async_copy(lbuf.at[0], link_out.at[0, 0, 1], out_sem.at[4]),
        pltpu.make_async_copy(lbuf.at[1], link_out.at[0, 0, 3], out_sem.at[5]),
        pltpu.make_async_copy(lbuf.at[2], link_out.at[1, 0, 0], out_sem.at[6]),
        pltpu.make_async_copy(dbuf, se_out, out_sem.at[7]),
    ]
    for c in outs[2:]:
        c.start()
    for c in outs:
        c.wait()


ANY = pl.BlockSpec(memory_space=pl.ANY)
VM = pl.BlockSpec(memory_space=pltpu.VMEM)


def local_call(diag_blocks, horizontal, vertical):
    b16 = pltpu.VMEM((N, N), BF16)
    f32 = pltpu.VMEM((N, N), F32)
    return pl.pallas_call(
        local_kernel,
        name="local",
        out_shape=(
            jax.ShapeDtypeStruct((2, 1, N, N), F32),
            jax.ShapeDtypeStruct((10, NB, NB), BF16),
            jax.ShapeDtypeStruct((26, NB, NB), BF16),
            jax.ShapeDtypeStruct((10, NB, NB), BF16),
            jax.ShapeDtypeStruct((2, 1, N, N), F32),
            jax.ShapeDtypeStruct((2, 1, 4, N, N), BF16),
            jax.ShapeDtypeStruct((2, N, N), F32),
        ),
        in_specs=[ANY] * 3,
        out_specs=(ANY, VM, VM, VM, ANY, ANY, ANY),
        scratch_shapes=[f32, f32]
        + [pltpu.VMEM((NB, 2 * NB), F32)] * 4
        + [pltpu.VMEM((NB, N), F32)] * 2
        + [f32, f32, b16, b16, pltpu.VMEM((2, N, N), F32)]
        + [pltpu.VMEM((2, 2, N, N), BF16)] * 2
        + [b16] * 6
        + [pltpu.VMEM((2, N, N), F32), pltpu.VMEM((3, N, N), BF16)]
        + [pltpu.SemaphoreType.DMA((6,)), pltpu.SemaphoreType.DMA((8,))],
        compiler_params=pltpu.CompilerParams(vmem_limit_bytes=56 << 20),
        cost_estimate=pl.CostEstimate(flops=60 * 10**9, bytes_accessed=20 << 20, transcendentals=0),
    )(diag_blocks, horizontal, vertical)


def unpack_lower(src_ref, dst_ref):
    zero = jnp.zeros((NB, NB), BF16)
    blocks = packed_blocks()
    for r in range(N // NB):
        for c in range(N // NB):
            value = src_ref[blocks.index((r, c))] if c <= r else zero
            dst_ref[r * NB : (r + 1) * NB, c * NB : (c + 1) * NB] = value


def symmetric(src_ref):
    blocks = packed_blocks()
    lines = []
    for r in range(N // NB):
        line = []
        for c in range(N // NB):
            if c <= r:
                line.append(src_ref[blocks.index((r, c))].astype(F32))
            else:
                line.append(src_ref[blocks.index((c, r))].astype(F32).T)
        lines.append(jnp.concatenate(line, 1))
    return jnp.concatenate(lines, 0)


def final_kernel(rinv, binv, rc2, rc3, bc0, bc2, bc3, c0, c1, from_left, from_above, schur_in, link_in, se,
                 schur_out, link_out, inv_a, inv_b, ra0, r2, r3, b0, b1, b2, b3, lbuf, sbuf, sem, ssem):
    loads = [pltpu.make_async_copy(schur_in, sbuf, ssem.at[0])]
    loads[0].start()
    unpack_lower(rinv, inv_a)
    solve_t(inv_a, c0, ra0)
    solve_n(inv_a, rc2, r2)
    solve_n(inv_a, rc3, r3)
    unpack_lower(binv, inv_b)
    solve_t(inv_b, bc0, b0)
    solve_t(inv_b, c1, b1)
    solve_n(inv_b, bc2, b2)
    solve_n(inv_b, bc3, b3)
    outs = []

    def link(slot, row, which, value):
        lbuf[slot] = (-value).astype(BF16)
        copy = pltpu.make_async_copy(lbuf.at[slot], link_out.at[row, 0, which], sem.at[slot])
        copy.start()
        outs.append(copy)

    link(0, 0, 0, dot(ra0[...], r2[...]))
    link(1, 0, 2, dot(ra0[...], r3[...]) + se[0])
    link(2, 1, 1, dot(b1[...], b3[...]))
    link(3, 1, 2, dot(b1[...], b2[...]) + se[1])
    loads[0].wait()
    sbuf[0, 0] = sbuf[0, 0] - (dot(ra0[...], ra0[...], 1, 1) + symmetric(from_above))
    sbuf[1, 0] = sbuf[1, 0] - (dot(b1[...], b1[...], 1, 1) + symmetric(from_left))
    copy = pltpu.make_async_copy(sbuf, schur_out, ssem.at[1])
    copy.start()
    outs.append(copy)
    side = jnp.concatenate(
        [
            jnp.concatenate([from_left[10 + 4 * r + c] for c in range(4)], 1)
            for r in range(4)
        ],
        0,
    )
    link(4, 1, 3, dot(b1[...], b0[...], 1, 1) + side.astype(F32))
    for c in outs:
        c.wait()


def final_call(*args):
    b16 = pltpu.VMEM((N, N), BF16)
    return pl.pallas_call(
        final_kernel,
        name="final",
        out_shape=(
            jax.ShapeDtypeStruct((2, 1, N, N), F32),
            jax.ShapeDtypeStruct((2, 1, 4, N, N), BF16),
        ),
        in_specs=[VM] * 11 + [ANY, ANY, VM],
        out_specs=(ANY, ANY),
        input_output_aliases={11: 0, 12: 1},
        scratch_shapes=[b16] * 9
        + [pltpu.VMEM((5, N, N), BF16), pltpu.VMEM((2, 1, N, N), F32)]
        + [pltpu.SemaphoreType.DMA((5,)), pltpu.SemaphoreType.DMA((2,))],
        compiler_params=pltpu.CompilerParams(vmem_limit_bytes=48 << 20),
        cost_estimate=pl.CostEstimate(flops=10 * 10**9, bytes_accessed=12 << 20, transcendentals=0),
    )(*args)


def passed(value, down, right):
    rows, cols = lax.axis_size("row"), lax.axis_size("col")
    if not right:
        return lax.ppermute(value, "row", [(i, (i + down) % rows) for i in range(rows)])
    if not down:
        return lax.ppermute(value, "col", [(i, (i + right) % cols) for i in range(cols)])
    pairs = [
        (r * cols + c, ((r + down) % rows) * cols + (c + right) % cols)
        for r in range(rows)
        for c in range(cols)
    ]
    return lax.ppermute(value, ("row", "col"), pairs)


def on_device(diag_blocks, horizontal, vertical):
    own2, own3, own0 = horizontal[0, 0], vertical[0, 0], horizontal[0, 1]
    below2 = passed(own2, -1, 0)
    below3 = passed(own3, -1, 0)
    right2 = passed(own2, 0, -1)
    right3 = passed(own3, 0, -1)
    below0 = passed(own0, -1, 1)
    factor, inverse, to_right, to_below, schur, links, southeast = local_call(
        diag_blocks, horizontal, vertical
    )
    below_inverse = passed(inverse, -1, 0)
    right_inverse = passed(inverse, 0, -1)
    from_left = passed(to_right, 0, 1)
    from_above = passed(to_below, 1, 0)
    schur, links = final_call(
        right_inverse, below_inverse, right2, right3, below0, below2, below3,
        own0, vertical[1, 0], from_left, from_above, schur, links, southeast,
    )
    return (factor, schur, links)


def solution(mesh):
    blocks = P("row", "col", None, None)
    return jax.shard_map(
        on_device,
        mesh=mesh,
        in_specs=(blocks, blocks, blocks),
        out_specs=(blocks, blocks, P("row", "col", None, None, None)),
        check_vma=False,
    )
```

```python
import jax
import jax.numpy as jnp
from jax import lax
from jax.experimental import pallas as pl
from jax.experimental.pallas import tpu as pltpu
from jax.sharding import PartitionSpec as P

N = 512
NB = 128
SB = 16
F32 = jnp.float32
BF16 = jnp.bfloat16


def dot(a, b, ca=1, cb=0):
    return lax.dot_general(a, b, (((ca,), (cb,)), ((), ())), preferred_element_type=F32)


def split(x):
    hi = x.astype(BF16)
    return hi, (x - hi.astype(F32)).astype(BF16)


def dot3(a, b, cb=0):
    ah, al = a
    bh, bl = b
    if cb == 1:
        return dot(ah, bh, 1, 1) + dot(al, bh, 1, 1) + dot(ah, bl, 1, 1)
    return dot(jnp.concatenate([ah, al], 1), jnp.concatenate([bh, bh], 0)) + dot(ah, bl)


def rows8(x, k):
    return jnp.broadcast_to(x[k : k + 1, :], (8, NB))


def eliminate(s, x_ref, p_ref, s_ref):
    k0 = SB * s
    row = lax.broadcasted_iota(jnp.int32, (8, NB), 0)
    xs = [[x_ref[k0 + 8 * h : k0 + 8 * h + 8, NB * w : NB * w + NB] for h in range(2)] for w in range(2)]
    cols = [
        [jnp.broadcast_to(xs[0][h][:, k0 + c : k0 + c + 1], (8, NB)) for h in range(2)]
        for c in range(SB)
    ]
    pivots = [jnp.ones((8, NB), F32) for _ in range(2)]
    saved = [[xs[w][h] for h in range(2)] for w in range(2)]
    for k in range(SB):
        kh, kr = divmod(k, 8)
        is_k = row == kr
        pivot = rows8(cols[k][kh], kr)
        inverse = 1.0 / pivot
        mult = [cols[k][h] * inverse for h in range(2)]
        mult[kh] = jnp.where(is_k, 0.0, mult[kh])
        for c in range(k + 1, SB):
            head = rows8(cols[c][kh], kr)
            cols[c] = [cols[c][h] - mult[h] * head for h in range(2)]
        pivots[kh] = jnp.where(is_k, pivot, pivots[kh])
        for w in range(2):
            saved[w][kh] = jnp.where(is_k, xs[w][kh], saved[w][kh])
            head = rows8(xs[w][kh], kr)
            xs[w] = [xs[w][h] - mult[h] * head for h in range(2)]
    for h in range(2):
        scale = lax.rsqrt(pivots[h])
        s_ref[k0 + 8 * h : k0 + 8 * h + 8, 0:NB] = scale
        s_ref[k0 + 8 * h : k0 + 8 * h + 8, NB : 2 * NB] = pivots[h] * scale
        for w in range(2):
            p_ref[k0 + 8 * h : k0 + 8 * h + 8, NB * w : NB * w + NB] = saved[w][h] * scale
    below = NB - k0 - SB
    if below:
        z = jnp.concatenate(
            [jnp.concatenate([xs[w][h] / pivots[h] for w in range(2)], 1) for h in range(2)], 0
        )
        zh, zl = split(z)

        def pad(v):
            parts = [v]
            if k0:
                parts.insert(0, jnp.zeros((k0, 2 * NB), BF16))
            parts.append(jnp.zeros((below, 2 * NB), BF16))
            return jnp.concatenate(parts, 0)

        a = split(x_ref[k0 + SB : NB, 0:NB])
        x_ref[k0 + SB : NB, :] = x_ref[k0 + SB : NB, :] - dot3(a, (pad(zh), pad(zl)))


def tiled(x):
    return jnp.concatenate([x] * (N // NB), 1)


def factor_all(g_refs, x_refs, p_refs, s_refs, w_refs, l_refs, e_refs, scale_refs):
    r_i = lax.broadcasted_iota(jnp.int32, (NB, NB), 0)
    c_i = lax.broadcasted_iota(jnp.int32, (NB, NB), 1)
    wide = lax.broadcasted_iota(jnp.int32, (NB, N), 1)
    for l_ref in l_refs:
        l_ref[...] = jnp.zeros_like(l_ref)

    def outer(o, carry):
        base = pl.multiple_of(o * NB, NB)
        here = pl.ds(base, NB)
        for g_ref, x_ref in zip(g_refs, x_refs):
            x_ref[:, 0:NB] = g_ref[here, here]
            x_ref[:, NB : 2 * NB] = jnp.where(r_i == c_i, 1.0, 0.0)
        for s in range(NB // SB):
            for x_ref, p_ref, s_ref in zip(x_refs, p_refs, s_refs):
                eliminate(s, x_ref, p_ref, s_ref)
        for m in range(2):
            p_ref, s_ref, w_ref = p_refs[m], s_refs[m], w_refs[m]
            l_refs[m][here, here] = jnp.where(r_i >= c_i, p_ref[:, 0:NB].T, 0.0)
            inverse = p_ref[:, NB : 2 * NB]
            w_ref[...] = dot3(split(inverse), split(g_refs[m][here, :]))
            w_ref[:, here] = inverse
            unit = w_ref[...] * tiled(s_ref[:, NB : 2 * NB])
            e_refs[m][here, :] = jnp.where(wide < base + NB, unit, 0.0).astype(BF16)
            scale_refs[m][here, :] = s_ref[:, 0:NB]
        for p in range(1, N // NB):
            rows = slice(p * NB, (p + 1) * NB)

            @pl.when(p > o)
            def _():
                for g_ref, p_ref, w_ref, l_ref in zip(g_refs, p_refs, w_refs, l_refs):
                    lower = dot3(split(g_ref[rows, here]), split(p_ref[:, NB : 2 * NB]), 1)
                    l_ref[rows, here] = lower
                    g_ref[rows, here] = jnp.zeros((NB, NB), F32)
                    g_ref[rows, :] = g_ref[rows, :] - dot3(split(lower), split(w_ref[...]))

        return carry

    lax.fori_loop(0, N // NB, outer, 0)


LOWER = [(r, c) for r in range(N // NB) for c in range(r)]
TAIL = 8 * NB
PACKED = TAIL + SB


def block(ref, r, c):
    return ref[r * NB : (r + 1) * NB, c * NB : (c + 1) * NB]


def at(first, b):
    return slice(first + b * NB, first + (b + 1) * NB)


def iotas():
    return (
        lax.broadcasted_iota(jnp.int32, (NB, NB), 0),
        lax.broadcasted_iota(jnp.int32, (NB, NB), 1),
    )


def pick_rows(rows):
    where = lax.broadcasted_iota(jnp.int32, (SB, NB), 0)
    tile = jnp.zeros((SB, NB), F32)
    for k, row in enumerate(rows):
        tile = jnp.where(where == k, jnp.broadcast_to(row, (SB, NB)), tile)
    return tile


def pack_unit(e_ref, scale_ref, dst_ref):
    r_i, c_i = iotas()
    for b, (r, c) in enumerate(LOWER):
        dst_ref[at(0, b), :] = block(e_ref, r, c)
    for k in range(2):
        one = block(e_ref, 2 * k, 2 * k).astype(F32)
        two = block(e_ref, 2 * k + 1, 2 * k + 1).astype(F32).T
        dst_ref[at(0, 6 + k), :] = jnp.where(r_i > c_i, one, jnp.where(r_i < c_i, two, 0.0)).astype(BF16)
    parts = [[], [], []]
    for k in range(N // NB):
        rest = scale_ref[k * NB : (k + 1) * NB, :].T[0:1, :]
        for part in parts:
            part.append(rest)
            rest = rest - rest.astype(BF16).astype(F32)
    dst_ref[TAIL:PACKED, :] = pick_rows(sum(parts, [])).astype(BF16)


def unpack_unit(src_ref, e_ref, scale_ref, row_ref):
    r_i, c_i = iotas()
    eye = jnp.where(r_i == c_i, 1.0, 0.0)
    zero = jnp.zeros((NB, NB), BF16)
    for b, (r, c) in enumerate(LOWER):
        e_ref[r * NB : (r + 1) * NB, c * NB : (c + 1) * NB] = src_ref[at(0, b), :]
        e_ref[c * NB : (c + 1) * NB, r * NB : (r + 1) * NB] = zero
    for k in range(2):
        pair = src_ref[at(0, 6 + k), :].astype(F32)
        for d, value in ((2 * k, pair), (2 * k + 1, pair.T)):
            e_ref[d * NB : (d + 1) * NB, d * NB : (d + 1) * NB] = jnp.where(r_i > c_i, value, eye).astype(BF16)
    tile = src_ref[TAIL:PACKED, :].astype(F32)
    for k in range(N // NB):
        row = tile[k : k + 1, :] + tile[4 + k : 5 + k, :] + tile[8 + k : 9 + k, :]
        row_ref[:, k * NB : (k + 1) * NB] = jnp.broadcast_to(row, (8, NB))
        scale_ref[k * NB : (k + 1) * NB, :] = jnp.broadcast_to(row, (NB, NB)).T


def scale_row(scale_ref, row_ref):
    for k in range(N // NB):
        row_ref[:, k * NB : (k + 1) * NB] = scale_ref[k * NB : (k + 1) * NB, :].T[0:8, :]


def pack_symmetric(value, dst_ref):
    r_i, c_i = iotas()
    for b, (r, c) in enumerate(LOWER):
        dst_ref[at(0, b), :] = block(value, r, c).astype(BF16)
    rows = []
    for k in range(2):
        two = block(value, 2 * k + 1, 2 * k + 1)
        dst_ref[at(0, 6 + k), :] = jnp.where(r_i >= c_i, block(value, 2 * k, 2 * k), two).astype(BF16)
        rows.append(jnp.sum(jnp.where(r_i == c_i, two, 0.0), 0, keepdims=True))
    dst_ref[TAIL:PACKED, :] = pick_rows(rows).astype(BF16)


def add_symmetric(src_ref, dst_ref):
    r_i, c_i = iotas()

    def sub(r, c, value):
        rows, cols = slice(r * NB, (r + 1) * NB), slice(c * NB, (c + 1) * NB)
        dst_ref[rows, cols] = dst_ref[rows, cols] - value

    for b, (r, c) in enumerate(LOWER):
        value = src_ref[at(0, b), :].astype(F32)
        sub(r, c, value)
        sub(c, r, value.T)
    tile = src_ref[TAIL:PACKED, :].astype(F32)
    for k in range(2):
        pair = src_ref[at(0, 6 + k), :].astype(F32)
        turned = pair.T
        sub(2 * k, 2 * k, jnp.where(r_i >= c_i, pair, turned))
        diagonal = jnp.broadcast_to(tile[k : k + 1, :], (NB, NB))
        two = jnp.where(r_i < c_i, pair, turned)
        sub(2 * k + 1, 2 * k + 1, jnp.where(r_i == c_i, diagonal, two))


def solve_t(e_ref, row_ref, c_ref, out_ref):
    h = N // 2
    row = row_ref[0:1, :]
    out_ref[:, 0:h] = (dot(c_ref[:, 0:h], e_ref[0:h, 0:h], 1, 1) * row[:, 0:h]).astype(BF16)
    out_ref[:, h:N] = (dot(c_ref[...], e_ref[h:N, :], 1, 1) * row[:, h:N]).astype(BF16)


def solve_n(e_ref, scale_ref, c_ref, out_ref):
    h = N // 2
    out_ref[0:h, :] = (dot(e_ref[0:h, 0:h], c_ref[0:h, :]) * tiled(scale_ref[0:h, :])).astype(BF16)
    out_ref[h:N, :] = (dot(e_ref[h:N, :], c_ref[...]) * tiled(scale_ref[h:N, :])).astype(BF16)


ANY = pl.BlockSpec(memory_space=pl.ANY)
VM = pl.BlockSpec(memory_space=pltpu.VMEM)
B16 = pltpu.VMEM((N, N), BF16)
WIDE = pltpu.VMEM((N, N), F32)


def shape(dims, kind):
    return jax.ShapeDtypeStruct(dims, kind)


def call(kernel, outs, in_specs, out_specs, scratch, flops, limit, aliases=None):
    return pl.pallas_call(
        kernel,
        out_shape=outs,
        in_specs=in_specs,
        out_specs=out_specs,
        scratch_shapes=scratch,
        input_output_aliases=aliases or {},
        compiler_params=pltpu.CompilerParams(vmem_limit_bytes=limit << 20),
        cost_estimate=pl.CostEstimate(flops=flops * 10**9, bytes_accessed=4 << 20, transcendentals=0),
    )


def factor_kernel(d_ref, l_out, e0, e1, scale0, scale1, packed,
                  g0, g1, x0, x1, p0, p1, s0, s1, w0, w1, l0, l1, in_sem, out_sem):
    copies = [
        pltpu.make_async_copy(d_ref.at[0, 0], g0, in_sem.at[0]),
        pltpu.make_async_copy(d_ref.at[1, 1], g1, in_sem.at[1]),
    ]
    for c in copies:
        c.start()
    for c in copies:
        c.wait()
    factor_all((g0, g1), (x0, x1), (p0, p1), (s0, s1), (w0, w1), (l0, l1), (e0, e1), (scale0, scale1))
    outs = [
        pltpu.make_async_copy(l0, l_out.at[0, 0], out_sem.at[0]),
        pltpu.make_async_copy(l1, l_out.at[1, 0], out_sem.at[1]),
    ]
    for c in outs:
        c.start()
    pack_unit(e0, scale0, packed)
    for c in outs:
        c.wait()


def factor_call(diag_blocks):
    half = pltpu.VMEM((NB, 2 * NB), F32)
    return call(
        factor_kernel,
        (shape((2, 1, N, N), F32), shape((N, N), BF16), shape((N, N), BF16),
         shape((N, NB), F32), shape((N, NB), F32), shape((PACKED, NB), BF16)),
        [ANY], (ANY, VM, VM, VM, VM, VM),
        [WIDE, WIDE] + [half] * 6 + [pltpu.VMEM((NB, N), F32)] * 2 + [WIDE, WIDE]
        + [pltpu.SemaphoreType.DMA((2,)), pltpu.SemaphoreType.DMA((2,))],
        60, 20,
    )(diag_blocks)


def local_kernel(d_ref, h_ref, v_ref, e0, e1, scale0, scale1, to_right, to_below, sbuf, dbuf, link_out,
                 hh, hv, y0, y1, y2, y3, z2, z3, lbuf, row1, in_sem, out_sem):
    copies = [
        pltpu.make_async_copy(h_ref, hh, in_sem.at[0]),
        pltpu.make_async_copy(v_ref, hv, in_sem.at[1]),
        pltpu.make_async_copy(d_ref.at[0, 1], sbuf.at[0], in_sem.at[2]),
        pltpu.make_async_copy(d_ref.at[1, 0], sbuf.at[1], in_sem.at[3]),
    ]
    for c in copies:
        c.start()
    for c in copies[:2]:
        c.wait()
    scale_row(scale1, row1)
    solve_n(e1, scale1, hh.at[1, 1], y2)
    solve_n(e1, scale1, hv.at[1, 1], y3)
    t2 = y2[...].T
    pack_symmetric(dot(t2, y2[...]), to_right)
    side = dot(t2, y3[...])
    for r in range(N // NB):
        for c in range(N // NB):
            to_right[at(PACKED, 4 * r + c), :] = block(side, r, c).astype(BF16)
    pack_symmetric(dot(y3[...].T, y3[...]), to_below)
    solve_t(e1, row1, hh.at[1, 0], y0)
    solve_t(e1, row1, hv.at[0, 1], y1)
    solve_n(e0, scale0, hh.at[0, 0], z2)
    solve_n(e0, scale0, hv.at[0, 0], z3)
    u2 = z2[...].T
    for c in copies[2:]:
        c.wait()
    outs = []

    def link(slot, row, which, value):
        lbuf[slot] = (-value).astype(BF16)
        copy = pltpu.make_async_copy(lbuf.at[slot], link_out.at[row, 0, which], out_sem.at[slot])
        copy.start()
        outs.append(copy)

    link(0, 0, 1, dot(y1[...], y3[...]))
    link(1, 0, 3, dot(u2, z3[...]) + dot(y1[...], y0[...], 1, 1))
    link(2, 1, 0, dot(y0[...], y2[...]))
    dbuf[0] = dot(y1[...], y2[...])
    dbuf[1] = dot(y0[...], y3[...])
    sbuf[0] = sbuf[0] - (dot(u2, z2[...]) + dot(y1[...], y1[...], 1, 1))
    sbuf[1] = sbuf[1] - (dot(z3[...].T, z3[...]) + dot(y0[...], y0[...], 1, 1))
    for c in outs:
        c.wait()


def local_call(*args):
    return call(
        local_kernel,
        (shape((PACKED + N * N // NB, NB), BF16), shape((PACKED, NB), BF16), shape((2, N, N), F32),
         shape((2, N, N), F32), shape((2, 1, 4, N, N), BF16)),
        [ANY] * 3 + [VM] * 4, (VM, VM, VM, VM, ANY),
        [pltpu.VMEM((2, 2, N, N), BF16)] * 2 + [B16] * 6
        + [pltpu.VMEM((3, N, N), BF16), pltpu.VMEM((8, N), F32)]
        + [pltpu.SemaphoreType.DMA((4,)), pltpu.SemaphoreType.DMA((3,))],
        12, 28,
    )(*args)


def across_kernel(h_ref, v_ref, rpack, bpack, rc, bc, bc0, se, schur_in, link_in, schur_out, sw, link_out,
                  inv_a, inv_b, c0, c1, ra0, r2, r3, b0, b1, b2, b3, scale_a, scale_b, row_a, row_b,
                  lbuf, in_sem, sem):
    loads = [
        pltpu.make_async_copy(h_ref.at[0, 1], c0, in_sem.at[0]),
        pltpu.make_async_copy(v_ref.at[1, 0], c1, in_sem.at[1]),
    ]
    for c in loads:
        c.start()
    unpack_unit(rpack, inv_a, scale_a, row_a)
    unpack_unit(bpack, inv_b, scale_b, row_b)
    for c in loads:
        c.wait()
    outs = []

    def link(slot, row, which, value):
        lbuf[slot] = (-value).astype(BF16)
        copy = pltpu.make_async_copy(lbuf.at[slot], link_out.at[row, 0, which], sem.at[slot])
        copy.start()
        outs.append(copy)

    solve_t(inv_a, row_a, c0, ra0)
    solve_n(inv_a, scale_a, rc.at[0], r2)
    solve_n(inv_a, scale_a, rc.at[1], r3)
    link(0, 0, 0, dot(ra0[...], r2[...]))
    link(1, 0, 2, dot(ra0[...], r3[...]) + se[0])
    solve_t(inv_b, row_b, c1, b1)
    solve_n(inv_b, scale_b, bc.at[1], b3)
    link(2, 1, 1, dot(b1[...], b3[...]))
    solve_n(inv_b, scale_b, bc.at[0], b2)
    link(3, 1, 2, dot(b1[...], b2[...]) + se[1])
    solve_t(inv_b, row_b, bc0, b0)
    schur_out[0] = schur_in[0] - dot(ra0[...], ra0[...], 1, 1)
    schur_out[1] = schur_in[1] - dot(b1[...], b1[...], 1, 1)
    sw[...] = dot(b1[...], b0[...], 1, 1)
    for c in outs:
        c.wait()


def across_call(*args):
    return call(
        across_kernel,
        (shape((2, N, N), F32), shape((N, N), F32), shape((2, 1, 4, N, N), BF16)),
        [ANY] * 2 + [VM] * 7 + [ANY], (VM, VM, ANY),
        [B16] * 11 + [pltpu.VMEM((N, NB), F32)] * 2 + [pltpu.VMEM((8, N), F32)] * 2
        + [pltpu.VMEM((4, N, N), BF16), pltpu.SemaphoreType.DMA((2,)), pltpu.SemaphoreType.DMA((4,))],
        10, 30, {9: 2},
    )(*args)


def last_kernel(from_left, from_above, schur_in, sw, link_in, schur_out, link_out, sbuf, lbuf, sem):
    lbuf[...] = jnp.concatenate(
        [
            jnp.concatenate(
                [
                    (-(block(sw, r, c) + from_left[at(PACKED, 4 * r + c), :].astype(F32))).astype(BF16)
                    for c in range(N // NB)
                ],
                1,
            )
            for r in range(N // NB)
        ],
        0,
    )
    outs = [
        pltpu.make_async_copy(lbuf, link_out.at[1, 0, 3], sem.at[0]),
        pltpu.make_async_copy(sbuf.at[0], schur_out.at[0, 0], sem.at[1]),
        pltpu.make_async_copy(sbuf.at[1], schur_out.at[1, 0], sem.at[2]),
    ]
    outs[0].start()
    for m, src in enumerate((from_above, from_left)):
        sbuf[m] = schur_in[m]
        add_symmetric(src, sbuf.at[m])
        outs[1 + m].start()
    for c in outs:
        c.wait()


def last_call(*args):
    return call(
        last_kernel,
        (shape((2, 1, N, N), F32), shape((2, 1, 4, N, N), BF16)),
        [VM] * 4 + [ANY], (ANY, ANY),
        [pltpu.VMEM((2, N, N), F32), B16, pltpu.SemaphoreType.DMA((3,))],
        2, 16, {4: 1},
    )(*args)


def passed(value, down, right):
    rows, cols = lax.axis_size("row"), lax.axis_size("col")
    if not right:
        return lax.ppermute(value, "row", [(i, (i + down) % rows) for i in range(rows)])
    if not down:
        return lax.ppermute(value, "col", [(i, (i + right) % cols) for i in range(cols)])
    pairs = [(r * cols + c, ((r + down) % rows) * cols + (c + right) % cols) for r in range(rows) for c in range(cols)]
    return lax.ppermute(value, ("row", "col"), pairs)


def on_device(diag_blocks, horizontal, vertical):
    pair = jnp.stack([horizontal[0, 0], vertical[0, 0]])
    below = passed(pair, -1, 0)
    right = passed(pair, 0, -1)
    below0 = passed(horizontal[0, 1], -1, 1)
    factor, e0, e1, scale0, scale1, packed = factor_call(diag_blocks)
    below_inverse = passed(packed, -1, 0)
    right_inverse = passed(packed, 0, -1)
    to_right, to_below, schur, southeast, links = local_call(diag_blocks, horizontal, vertical, e0, e1, scale0, scale1)
    from_left = passed(to_right, 0, 1)
    from_above = passed(to_below, 1, 0)
    schur, southwest, links = across_call(
        horizontal, vertical, right_inverse, below_inverse, right, below, below0,
        southeast, schur, links,
    )
    schur, links = last_call(from_left, from_above, schur, southwest, links)
    return (factor, schur, links)


def solution(mesh):
    blocks = P("row", "col", None, None)
    return jax.shard_map(
        on_device,
        mesh=mesh,
        in_specs=(blocks, blocks, blocks),
        out_specs=(blocks, blocks, P("row", "col", None, None, None)),
        check_vma=False,
    )
```

```python
import jax
import jax.numpy as jnp
from jax import lax
from jax.experimental import pallas as pl
from jax.experimental.pallas import tpu as pltpu
from jax.sharding import PartitionSpec as P

N = 512
NB = 128
SB = 16
F32 = jnp.float32
BF16 = jnp.bfloat16


def dot(a, b, ca=1, cb=0):
    return lax.dot_general(a, b, (((ca,), (cb,)), ((), ())), preferred_element_type=F32)


def split(x):
    hi = x.astype(BF16)
    return hi, (x - hi.astype(F32)).astype(BF16)


def dot3(a, b, cb=0):
    ah, al = a
    bh, bl = b
    if cb == 1:
        return dot(ah, bh, 1, 1) + dot(al, bh, 1, 1) + dot(ah, bl, 1, 1)
    return dot(jnp.concatenate([ah, al], 1), jnp.concatenate([bh, bh], 0)) + dot(ah, bl)


def rows8(x, k):
    return jnp.broadcast_to(x[k : k + 1, :], (8, NB))


def eliminate(s, x_ref, p_ref, s_ref):
    k0 = SB * s
    row = lax.broadcasted_iota(jnp.int32, (8, NB), 0)
    xs = [[x_ref[k0 + 8 * h : k0 + 8 * h + 8, NB * w : NB * w + NB] for h in range(2)] for w in range(2)]
    cols = [
        [jnp.broadcast_to(xs[0][h][:, k0 + c : k0 + c + 1], (8, NB)) for h in range(2)]
        for c in range(SB)
    ]
    pivots = [jnp.ones((8, NB), F32) for _ in range(2)]
    saved = [[xs[w][h] for h in range(2)] for w in range(2)]
    for k in range(SB):
        kh, kr = divmod(k, 8)
        is_k = row == kr
        pivot = rows8(cols[k][kh], kr)
        inverse = 1.0 / pivot
        mult = [cols[k][h] * inverse for h in range(2)]
        mult[kh] = jnp.where(is_k, 0.0, mult[kh])
        for c in range(k + 1, SB):
            head = rows8(cols[c][kh], kr)
            cols[c] = [cols[c][h] - mult[h] * head for h in range(2)]
        pivots[kh] = jnp.where(is_k, pivot, pivots[kh])
        for w in range(2):
            saved[w][kh] = jnp.where(is_k, xs[w][kh], saved[w][kh])
            head = rows8(xs[w][kh], kr)
            xs[w] = [xs[w][h] - mult[h] * head for h in range(2)]
    for h in range(2):
        scale = lax.rsqrt(pivots[h])
        s_ref[k0 + 8 * h : k0 + 8 * h + 8, 0:NB] = scale
        s_ref[k0 + 8 * h : k0 + 8 * h + 8, NB : 2 * NB] = pivots[h] * scale
        for w in range(2):
            p_ref[k0 + 8 * h : k0 + 8 * h + 8, NB * w : NB * w + NB] = saved[w][h] * scale
    below = NB - k0 - SB
    if below:
        z = jnp.concatenate(
            [jnp.concatenate([xs[w][h] / pivots[h] for w in range(2)], 1) for h in range(2)], 0
        )
        zh, zl = split(z)

        def pad(v):
            parts = [v]
            if k0:
                parts.insert(0, jnp.zeros((k0, 2 * NB), BF16))
            parts.append(jnp.zeros((below, 2 * NB), BF16))
            return jnp.concatenate(parts, 0)

        a = split(x_ref[k0 + SB : NB, 0:NB])
        x_ref[k0 + SB : NB, :] = x_ref[k0 + SB : NB, :] - dot3(a, (pad(zh), pad(zl)))


def tiled(x):
    return jnp.concatenate([x] * (N // NB), 1)


def factor_steps(first, last, g_refs, x_refs, p_refs, s_refs, w_refs, l_refs, e_refs, scale_refs):
    r_i = lax.broadcasted_iota(jnp.int32, (NB, NB), 0)
    c_i = lax.broadcasted_iota(jnp.int32, (NB, NB), 1)
    wide = lax.broadcasted_iota(jnp.int32, (NB, N), 1)
    for l_ref in l_refs:
        l_ref[...] = jnp.zeros_like(l_ref)

    def outer(o, carry):
        base = pl.multiple_of(o * NB, NB)
        here = pl.ds(base, NB)
        for g_ref, x_ref in zip(g_refs, x_refs):
            x_ref[:, 0:NB] = g_ref[here, here]
            x_ref[:, NB : 2 * NB] = jnp.where(r_i == c_i, 1.0, 0.0)
        for s in range(NB // SB):
            for x_ref, p_ref, s_ref in zip(x_refs, p_refs, s_refs):
                eliminate(s, x_ref, p_ref, s_ref)
        for m in range(2):
            p_ref, s_ref, w_ref = p_refs[m], s_refs[m], w_refs[m]
            l_refs[m][here, here] = jnp.where(r_i >= c_i, p_ref[:, 0:NB].T, 0.0)
            inverse = p_ref[:, NB : 2 * NB]
            w_ref[...] = dot3(split(inverse), split(g_refs[m][here, :]))
            w_ref[:, here] = inverse
            unit = w_ref[...] * tiled(s_ref[:, NB : 2 * NB])
            e_refs[m][here, :] = jnp.where(wide < base + NB, unit, 0.0).astype(BF16)
            scale_refs[m][here, :] = s_ref[:, 0:NB]
        for p in range(first + 1, N // NB):
            rows = slice(p * NB, (p + 1) * NB)

            @pl.when(p > o)
            def _():
                for g_ref, p_ref, w_ref, l_ref in zip(g_refs, p_refs, w_refs, l_refs):
                    lower = dot3(split(g_ref[rows, here]), split(p_ref[:, NB : 2 * NB]), 1)
                    l_ref[rows, here] = lower
                    g_ref[rows, here] = jnp.zeros((NB, NB), F32)
                    g_ref[rows, :] = g_ref[rows, :] - dot3(split(lower), split(w_ref[...]))

        return carry

    lax.fori_loop(first, last, outer, 0)


LOWER = [(r, c) for r in range(N // NB) for c in range(r)]
TAIL = 8 * NB
PACKED = TAIL + SB


def block(ref, r, c):
    return ref[r * NB : (r + 1) * NB, c * NB : (c + 1) * NB]


def at(first, b):
    return slice(first + b * NB, first + (b + 1) * NB)


def iotas():
    return (
        lax.broadcasted_iota(jnp.int32, (NB, NB), 0),
        lax.broadcasted_iota(jnp.int32, (NB, NB), 1),
    )


def pick_rows(rows):
    where = lax.broadcasted_iota(jnp.int32, (SB, NB), 0)
    tile = jnp.zeros((SB, NB), F32)
    for k, row in enumerate(rows):
        tile = jnp.where(where == k, jnp.broadcast_to(row, (SB, NB)), tile)
    return tile


def pack_unit(e_ref, scale_ref, dst_ref):
    r_i, c_i = iotas()
    for b, (r, c) in enumerate(LOWER):
        dst_ref[at(0, b), :] = block(e_ref, r, c)
    for k in range(2):
        one = block(e_ref, 2 * k, 2 * k).astype(F32)
        two = block(e_ref, 2 * k + 1, 2 * k + 1).astype(F32).T
        dst_ref[at(0, 6 + k), :] = jnp.where(r_i > c_i, one, jnp.where(r_i < c_i, two, 0.0)).astype(BF16)
    parts = [[], [], []]
    for k in range(N // NB):
        rest = scale_ref[k * NB : (k + 1) * NB, :].T[0:1, :]
        for part in parts:
            part.append(rest)
            rest = rest - rest.astype(BF16).astype(F32)
    dst_ref[TAIL:PACKED, :] = pick_rows(sum(parts, [])).astype(BF16)


def unpack_unit(src_ref, e_ref, scale_ref, row_ref):
    r_i, c_i = iotas()
    eye = jnp.where(r_i == c_i, 1.0, 0.0)
    zero = jnp.zeros((NB, NB), BF16)
    for b, (r, c) in enumerate(LOWER):
        e_ref[r * NB : (r + 1) * NB, c * NB : (c + 1) * NB] = src_ref[at(0, b), :]
        e_ref[c * NB : (c + 1) * NB, r * NB : (r + 1) * NB] = zero
    for k in range(2):
        pair = src_ref[at(0, 6 + k), :].astype(F32)
        for d, value in ((2 * k, pair), (2 * k + 1, pair.T)):
            e_ref[d * NB : (d + 1) * NB, d * NB : (d + 1) * NB] = jnp.where(r_i > c_i, value, eye).astype(BF16)
    tile = src_ref[TAIL:PACKED, :].astype(F32)
    for k in range(N // NB):
        row = tile[k : k + 1, :] + tile[4 + k : 5 + k, :] + tile[8 + k : 9 + k, :]
        row_ref[:, k * NB : (k + 1) * NB] = jnp.broadcast_to(row, (8, NB))
        scale_ref[k * NB : (k + 1) * NB, :] = jnp.broadcast_to(row, (NB, NB)).T


def scale_row(scale_ref, row_ref):
    for k in range(N // NB):
        row_ref[:, k * NB : (k + 1) * NB] = scale_ref[k * NB : (k + 1) * NB, :].T[0:8, :]


def pack_symmetric(value, dst_ref):
    r_i, c_i = iotas()
    for b, (r, c) in enumerate(LOWER):
        dst_ref[at(0, b), :] = block(value, r, c).astype(BF16)
    rows = []
    for k in range(2):
        two = block(value, 2 * k + 1, 2 * k + 1)
        dst_ref[at(0, 6 + k), :] = jnp.where(r_i >= c_i, block(value, 2 * k, 2 * k), two).astype(BF16)
        rows.append(jnp.sum(jnp.where(r_i == c_i, two, 0.0), 0, keepdims=True))
    dst_ref[TAIL:PACKED, :] = pick_rows(rows).astype(BF16)


def add_symmetric(src_ref, dst_ref):
    r_i, c_i = iotas()

    def sub(r, c, value):
        rows, cols = slice(r * NB, (r + 1) * NB), slice(c * NB, (c + 1) * NB)
        dst_ref[rows, cols] = dst_ref[rows, cols] - value

    for b, (r, c) in enumerate(LOWER):
        value = src_ref[at(0, b), :].astype(F32)
        sub(r, c, value)
        sub(c, r, value.T)
    tile = src_ref[TAIL:PACKED, :].astype(F32)
    for k in range(2):
        pair = src_ref[at(0, 6 + k), :].astype(F32)
        turned = pair.T
        sub(2 * k, 2 * k, jnp.where(r_i >= c_i, pair, turned))
        diagonal = jnp.broadcast_to(tile[k : k + 1, :], (NB, NB))
        two = jnp.where(r_i < c_i, pair, turned)
        sub(2 * k + 1, 2 * k + 1, jnp.where(r_i == c_i, diagonal, two))


def solve_t(e_ref, row_ref, c_ref, out_ref):
    h = N // 2
    row = row_ref[0:1, :]
    out_ref[:, 0:h] = (dot(c_ref[:, 0:h], e_ref[0:h, 0:h], 1, 1) * row[:, 0:h]).astype(BF16)
    out_ref[:, h:N] = (dot(c_ref[...], e_ref[h:N, :], 1, 1) * row[:, h:N]).astype(BF16)


def solve_n(e_ref, scale_ref, c_ref, out_ref):
    h = N // 2
    out_ref[0:h, :] = (dot(e_ref[0:h, 0:h], c_ref[0:h, :]) * tiled(scale_ref[0:h, :])).astype(BF16)
    out_ref[h:N, :] = (dot(e_ref[h:N, :], c_ref[...]) * tiled(scale_ref[h:N, :])).astype(BF16)


ANY = pl.BlockSpec(memory_space=pl.ANY)
VM = pl.BlockSpec(memory_space=pltpu.VMEM)
B16 = pltpu.VMEM((N, N), BF16)
WIDE = pltpu.VMEM((N, N), F32)


def shape(dims, kind):
    return jax.ShapeDtypeStruct(dims, kind)


def call(kernel, outs, in_specs, out_specs, scratch, flops, limit, aliases=None):
    return pl.pallas_call(
        kernel,
        out_shape=outs,
        in_specs=in_specs,
        out_specs=out_specs,
        scratch_shapes=scratch,
        input_output_aliases=aliases or {},
        compiler_params=pltpu.CompilerParams(vmem_limit_bytes=limit << 20),
        cost_estimate=pl.CostEstimate(flops=flops * 10**9, bytes_accessed=4 << 20, transcendentals=0),
    )


H = N // 2
HALF = [pltpu.VMEM((NB, 2 * NB), F32)] * 6 + [pltpu.VMEM((NB, N), F32)] * 2
DMA2 = pltpu.SemaphoreType.DMA((2,))


def first_kernel(d_ref, l_out, ga, gb, ea, eb, sa, sb,
                 x0, x1, p0, p1, s0, s1, w0, w1, g0, g1, l0, l1, e0, e1, scale0, scale1, in_sem, out_sem):
    copies = [
        pltpu.make_async_copy(d_ref.at[0, 0], g0, in_sem.at[0]),
        pltpu.make_async_copy(d_ref.at[1, 1], g1, in_sem.at[1]),
    ]
    for c in copies:
        c.start()
    for c in copies:
        c.wait()
    factor_steps(0, 2, (g0, g1), (x0, x1), (p0, p1), (s0, s1), (w0, w1), (l0, l1), (e0, e1), (scale0, scale1))
    outs = [
        pltpu.make_async_copy(l_ref.at[:, 0:H], l_out.at[m, 0, :, 0:H], out_sem.at[m])
        for m, l_ref in enumerate((l0, l1))
    ]
    for c in outs:
        c.start()
    for dst, src in ((ga, g0), (gb, g1)):
        dst[...] = src[H:N, :]
    for dst, src in ((ea, e0), (eb, e1), (sa, scale0), (sb, scale1)):
        dst[...] = src[0:H, :]
    for c in outs:
        c.wait()


def second_kernel(l_in, ga, gb, ea, eb, sa, sb, l_out, e0, e1, scale0, scale1, packed,
                  x0, x1, p0, p1, s0, s1, w0, w1, g0, g1, l0, l1, out_sem):
    for dst, src in ((g0, ga), (g1, gb)):
        dst[H:N, :] = src[...]
    for dst, src in ((e0, ea), (e1, eb), (scale0, sa), (scale1, sb)):
        dst[0:H, :] = src[...]
    factor_steps(2, 4, (g0, g1), (x0, x1), (p0, p1), (s0, s1), (w0, w1), (l0, l1), (e0, e1), (scale0, scale1))
    outs = [
        pltpu.make_async_copy(l_ref.at[:, H:N], l_out.at[m, 0, :, H:N], out_sem.at[m])
        for m, l_ref in enumerate((l0, l1))
    ]
    for c in outs:
        c.start()
    pack_unit(e0, scale0, packed)
    for c in outs:
        c.wait()


STATE = (
    shape((H, N), F32), shape((H, N), F32), shape((H, N), BF16), shape((H, N), BF16),
    shape((H, NB), F32), shape((H, NB), F32),
)
COL = pltpu.VMEM((N, NB), F32)


def first_call(diag_blocks):
    return call(
        first_kernel, (shape((2, 1, N, N), F32),) + STATE, [ANY], (ANY,) + (VM,) * 6,
        HALF + [WIDE] * 4 + [B16, B16, COL, COL, DMA2, DMA2], 30, 20,
    )(diag_blocks)


def second_call(*args):
    return call(
        second_kernel,
        (shape((2, 1, N, N), F32), shape((N, N), BF16), shape((N, N), BF16),
         shape((N, NB), F32), shape((N, NB), F32), shape((PACKED, NB), BF16)),
        [ANY] + [VM] * 6, (ANY, VM, VM, VM, VM, VM), HALF + [WIDE] * 4 + [DMA2], 30, 20, {0: 0},
    )(*args)


def local_kernel(d_ref, h_ref, v_ref, e0, e1, scale0, scale1, to_right, to_below, sbuf, dbuf, link_out,
                 hh, hv, y0, y1, y2, y3, z2, z3, lbuf, row1, in_sem, out_sem):
    copies = [
        pltpu.make_async_copy(h_ref, hh, in_sem.at[0]),
        pltpu.make_async_copy(v_ref, hv, in_sem.at[1]),
        pltpu.make_async_copy(d_ref.at[0, 1], sbuf.at[0], in_sem.at[2]),
        pltpu.make_async_copy(d_ref.at[1, 0], sbuf.at[1], in_sem.at[3]),
    ]
    for c in copies:
        c.start()
    for c in copies[:2]:
        c.wait()
    scale_row(scale1, row1)
    solve_n(e1, scale1, hh.at[1, 1], y2)
    solve_n(e1, scale1, hv.at[1, 1], y3)
    t2 = y2[...].T
    pack_symmetric(dot(t2, y2[...]), to_right)
    side = dot(t2, y3[...])
    for r in range(N // NB):
        for c in range(N // NB):
            to_right[at(PACKED, 4 * r + c), :] = block(side, r, c).astype(BF16)
    pack_symmetric(dot(y3[...].T, y3[...]), to_below)
    solve_t(e1, row1, hh.at[1, 0], y0)
    solve_t(e1, row1, hv.at[0, 1], y1)
    solve_n(e0, scale0, hh.at[0, 0], z2)
    solve_n(e0, scale0, hv.at[0, 0], z3)
    u2 = z2[...].T
    for c in copies[2:]:
        c.wait()
    outs = []

    def link(slot, row, which, value):
        lbuf[slot] = (-value).astype(BF16)
        copy = pltpu.make_async_copy(lbuf.at[slot], link_out.at[row, 0, which], out_sem.at[slot])
        copy.start()
        outs.append(copy)

    link(0, 0, 1, dot(y1[...], y3[...]))
    link(1, 0, 3, dot(u2, z3[...]) + dot(y1[...], y0[...], 1, 1))
    link(2, 1, 0, dot(y0[...], y2[...]))
    dbuf[0] = dot(y1[...], y2[...])
    dbuf[1] = dot(y0[...], y3[...])
    sbuf[0] = sbuf[0] - (dot(u2, z2[...]) + dot(y1[...], y1[...], 1, 1))
    sbuf[1] = sbuf[1] - (dot(z3[...].T, z3[...]) + dot(y0[...], y0[...], 1, 1))
    for c in outs:
        c.wait()


def local_call(*args):
    return call(
        local_kernel,
        (shape((PACKED + N * N // NB, NB), BF16), shape((PACKED, NB), BF16), shape((2, N, N), F32),
         shape((2, N, N), F32), shape((2, 1, 4, N, N), BF16)),
        [ANY] * 3 + [VM] * 4, (VM, VM, VM, VM, ANY),
        [pltpu.VMEM((2, 2, N, N), BF16)] * 2 + [B16] * 6
        + [pltpu.VMEM((3, N, N), BF16), pltpu.VMEM((8, N), F32)]
        + [pltpu.SemaphoreType.DMA((4,)), pltpu.SemaphoreType.DMA((3,))],
        12, 28,
    )(*args)


def across_kernel(h_ref, v_ref, rpack, bpack, rc, bc, bc0, se, schur_in, link_in, schur_out, sw, link_out,
                  inv_a, inv_b, c0, c1, ra0, r2, r3, b0, b1, b2, b3, scale_a, scale_b, row_a, row_b,
                  lbuf, in_sem, sem):
    loads = [
        pltpu.make_async_copy(h_ref.at[0, 1], c0, in_sem.at[0]),
        pltpu.make_async_copy(v_ref.at[1, 0], c1, in_sem.at[1]),
    ]
    for c in loads:
        c.start()
    unpack_unit(rpack, inv_a, scale_a, row_a)
    unpack_unit(bpack, inv_b, scale_b, row_b)
    for c in loads:
        c.wait()
    outs = []

    def link(slot, row, which, value):
        lbuf[slot] = (-value).astype(BF16)
        copy = pltpu.make_async_copy(lbuf.at[slot], link_out.at[row, 0, which], sem.at[slot])
        copy.start()
        outs.append(copy)

    solve_t(inv_a, row_a, c0, ra0)
    solve_n(inv_a, scale_a, rc.at[0], r2)
    solve_n(inv_a, scale_a, rc.at[1], r3)
    link(0, 0, 0, dot(ra0[...], r2[...]))
    link(1, 0, 2, dot(ra0[...], r3[...]) + se[0])
    solve_t(inv_b, row_b, c1, b1)
    solve_n(inv_b, scale_b, bc.at[1], b3)
    link(2, 1, 1, dot(b1[...], b3[...]))
    solve_n(inv_b, scale_b, bc.at[0], b2)
    link(3, 1, 2, dot(b1[...], b2[...]) + se[1])
    solve_t(inv_b, row_b, bc0, b0)
    schur_out[0] = schur_in[0] - dot(ra0[...], ra0[...], 1, 1)
    schur_out[1] = schur_in[1] - dot(b1[...], b1[...], 1, 1)
    sw[...] = dot(b1[...], b0[...], 1, 1)
    for c in outs:
        c.wait()


def across_call(*args):
    return call(
        across_kernel,
        (shape((2, N, N), F32), shape((N, N), F32), shape((2, 1, 4, N, N), BF16)),
        [ANY] * 2 + [VM] * 7 + [ANY], (VM, VM, ANY),
        [B16] * 11 + [pltpu.VMEM((N, NB), F32)] * 2 + [pltpu.VMEM((8, N), F32)] * 2
        + [pltpu.VMEM((4, N, N), BF16), pltpu.SemaphoreType.DMA((2,)), pltpu.SemaphoreType.DMA((4,))],
        10, 30, {9: 2},
    )(*args)


def last_kernel(from_left, from_above, schur_in, sw, link_in, schur_out, link_out, sbuf, lbuf, sem):
    lbuf[...] = jnp.concatenate(
        [
            jnp.concatenate(
                [
                    (-(block(sw, r, c) + from_left[at(PACKED, 4 * r + c), :].astype(F32))).astype(BF16)
                    for c in range(N // NB)
                ],
                1,
            )
            for r in range(N // NB)
        ],
        0,
    )
    outs = [
        pltpu.make_async_copy(lbuf, link_out.at[1, 0, 3], sem.at[0]),
        pltpu.make_async_copy(sbuf.at[0], schur_out.at[0, 0], sem.at[1]),
        pltpu.make_async_copy(sbuf.at[1], schur_out.at[1, 0], sem.at[2]),
    ]
    outs[0].start()
    for m, src in enumerate((from_above, from_left)):
        sbuf[m] = schur_in[m]
        add_symmetric(src, sbuf.at[m])
        outs[1 + m].start()
    for c in outs:
        c.wait()


def last_call(*args):
    return call(
        last_kernel,
        (shape((2, 1, N, N), F32), shape((2, 1, 4, N, N), BF16)),
        [VM] * 4 + [ANY], (ANY, ANY),
        [pltpu.VMEM((2, N, N), F32), B16, pltpu.SemaphoreType.DMA((3,))],
        2, 16, {4: 1},
    )(*args)


def passed(value, down, right):
    rows, cols = lax.axis_size("row"), lax.axis_size("col")
    pairs = [
        (r * cols + c, ((r + down) % rows) * cols + (c + right) % cols)
        for r in range(rows)
        for c in range(cols)
    ]
    return lax.ppermute(value, ("row", "col"), pairs)


def on_device(diag_blocks, horizontal, vertical):
    pair = jnp.stack([horizontal[0, 0], vertical[0, 0]])
    right = passed(pair, 0, -1)
    below0 = passed(horizontal[0, 1], -1, 1)
    state = first_call(diag_blocks)
    below = passed(right, -1, 1)
    factor, e0, e1, scale0, scale1, packed = second_call(*state)
    right_inverse = passed(packed, 0, -1)
    to_right, to_below, schur, southeast, links = local_call(diag_blocks, horizontal, vertical, e0, e1, scale0, scale1)
    below_inverse = passed(right_inverse, -1, 1)
    from_left = passed(to_right, 0, 1)
    from_above = passed(to_below, 1, 0)
    schur, southwest, links = across_call(
        horizontal, vertical, right_inverse, below_inverse, right, below, below0,
        southeast, schur, links,
    )
    schur, links = last_call(from_left, from_above, schur, southwest, links)
    return (factor, schur, links)


def solution(mesh):
    blocks = P("row", "col", None, None)
    return jax.shard_map(
        on_device,
        mesh=mesh,
        in_specs=(blocks, blocks, blocks),
        out_specs=(blocks, blocks, P("row", "col", None, None, None)),
        check_vma=False,
    )
```

```python
import jax
import jax.numpy as jnp
from jax import lax
from jax.experimental import pallas as pl
from jax.experimental.pallas import tpu as pltpu
from jax.sharding import PartitionSpec as P

N = 512
NB = 128
SB = 16
F32 = jnp.float32
BF16 = jnp.bfloat16


def dot(a, b, ca=1, cb=0):
    return lax.dot_general(a, b, (((ca,), (cb,)), ((), ())), preferred_element_type=F32)


def split(x):
    hi = x.astype(BF16)
    return hi, (x - hi.astype(F32)).astype(BF16)


def dot3(a, b, cb=0):
    ah, al = a
    bh, bl = b
    if cb == 1:
        return dot(ah, bh, 1, 1) + dot(al, bh, 1, 1) + dot(ah, bl, 1, 1)
    return dot(jnp.concatenate([ah, al], 1), jnp.concatenate([bh, bh], 0)) + dot(ah, bl)


def rows8(x, k):
    return jnp.broadcast_to(x[k : k + 1, :], (8, NB))


def eliminate(s, x_ref, p_ref, s_ref):
    k0 = SB * s
    row = lax.broadcasted_iota(jnp.int32, (8, NB), 0)
    xs = [[x_ref[k0 + 8 * h : k0 + 8 * h + 8, NB * w : NB * w + NB] for h in range(2)] for w in range(2)]
    cols = [
        [jnp.broadcast_to(xs[0][h][:, k0 + c : k0 + c + 1], (8, NB)) for h in range(2)]
        for c in range(SB)
    ]
    pivots = [jnp.ones((8, NB), F32) for _ in range(2)]
    saved = [[xs[w][h] for h in range(2)] for w in range(2)]
    for k in range(SB):
        kh, kr = divmod(k, 8)
        is_k = row == kr
        pivot = rows8(cols[k][kh], kr)
        inverse = 1.0 / pivot
        mult = [cols[k][h] * inverse for h in range(2)]
        mult[kh] = jnp.where(is_k, 0.0, mult[kh])
        for c in range(k + 1, SB):
            head = rows8(cols[c][kh], kr)
            cols[c] = [cols[c][h] - mult[h] * head for h in range(2)]
        pivots[kh] = jnp.where(is_k, pivot, pivots[kh])
        for w in range(2):
            saved[w][kh] = jnp.where(is_k, xs[w][kh], saved[w][kh])
            head = rows8(xs[w][kh], kr)
            xs[w] = [xs[w][h] - mult[h] * head for h in range(2)]
    for h in range(2):
        scale = lax.rsqrt(pivots[h])
        s_ref[k0 + 8 * h : k0 + 8 * h + 8, 0:NB] = scale
        s_ref[k0 + 8 * h : k0 + 8 * h + 8, NB : 2 * NB] = pivots[h] * scale
        for w in range(2):
            p_ref[k0 + 8 * h : k0 + 8 * h + 8, NB * w : NB * w + NB] = saved[w][h] * scale
    below = NB - k0 - SB
    if below:
        z = jnp.concatenate(
            [jnp.concatenate([xs[w][h] / pivots[h] for w in range(2)], 1) for h in range(2)], 0
        )
        zh, zl = split(z)

        def pad(v):
            parts = [v]
            if k0:
                parts.insert(0, jnp.zeros((k0, 2 * NB), BF16))
            parts.append(jnp.zeros((below, 2 * NB), BF16))
            return jnp.concatenate(parts, 0)

        a = split(x_ref[k0 + SB : NB, 0:NB])
        x_ref[k0 + SB : NB, :] = x_ref[k0 + SB : NB, :] - dot3(a, (pad(zh), pad(zl)))


def tiled(x):
    return jnp.concatenate([x] * (N // NB), 1)


def factor_steps(first, last, g_refs, x_refs, p_refs, s_refs, w_refs, l_refs, e_refs, scale_refs):
    r_i = lax.broadcasted_iota(jnp.int32, (NB, NB), 0)
    c_i = lax.broadcasted_iota(jnp.int32, (NB, NB), 1)
    wide = lax.broadcasted_iota(jnp.int32, (NB, N), 1)
    for l_ref in l_refs:
        l_ref[...] = jnp.zeros_like(l_ref)

    def outer(o, carry):
        base = pl.multiple_of(o * NB, NB)
        here = pl.ds(base, NB)
        for g_ref, x_ref in zip(g_refs, x_refs):
            x_ref[:, 0:NB] = g_ref[here, here]
            x_ref[:, NB : 2 * NB] = jnp.where(r_i == c_i, 1.0, 0.0)
        for s in range(NB // SB):
            for x_ref, p_ref, s_ref in zip(x_refs, p_refs, s_refs):
                eliminate(s, x_ref, p_ref, s_ref)
        for m in range(2):
            p_ref, s_ref, w_ref = p_refs[m], s_refs[m], w_refs[m]
            l_refs[m][here, here] = jnp.where(r_i >= c_i, p_ref[:, 0:NB].T, 0.0)
            inverse = p_ref[:, NB : 2 * NB]
            w_ref[...] = dot3(split(inverse), split(g_refs[m][here, :]))
            w_ref[:, here] = inverse
            unit = w_ref[...] * tiled(s_ref[:, NB : 2 * NB])
            e_refs[m][here, :] = jnp.where(wide < base + NB, unit, 0.0).astype(BF16)
            scale_refs[m][here, :] = s_ref[:, 0:NB]
        for p in range(first + 1, N // NB):
            rows = slice(p * NB, (p + 1) * NB)

            @pl.when(p > o)
            def _():
                for g_ref, p_ref, w_ref, l_ref in zip(g_refs, p_refs, w_refs, l_refs):
                    lower = dot3(split(g_ref[rows, here]), split(p_ref[:, NB : 2 * NB]), 1)
                    l_ref[rows, here] = lower
                    g_ref[rows, here] = jnp.zeros((NB, NB), F32)
                    g_ref[rows, :] = g_ref[rows, :] - dot3(split(lower), split(w_ref[...]))

        return carry

    lax.fori_loop(first, last, outer, 0)


LOWER = [(r, c) for r in range(N // NB) for c in range(r)]
TAIL = 8 * NB
PACKED = TAIL + SB


def block(ref, r, c):
    return ref[r * NB : (r + 1) * NB, c * NB : (c + 1) * NB]


def at(first, b):
    return slice(first + b * NB, first + (b + 1) * NB)


def iotas():
    return (
        lax.broadcasted_iota(jnp.int32, (NB, NB), 0),
        lax.broadcasted_iota(jnp.int32, (NB, NB), 1),
    )


def pick_rows(rows):
    where = lax.broadcasted_iota(jnp.int32, (SB, NB), 0)
    tile = jnp.zeros((SB, NB), F32)
    for k, row in enumerate(rows):
        tile = jnp.where(where == k, jnp.broadcast_to(row, (SB, NB)), tile)
    return tile


def pack_unit(e_ref, scale_ref, dst_ref):
    r_i, c_i = iotas()
    for b, (r, c) in enumerate(LOWER):
        dst_ref[at(0, b), :] = block(e_ref, r, c)
    for k in range(2):
        one = block(e_ref, 2 * k, 2 * k).astype(F32)
        two = block(e_ref, 2 * k + 1, 2 * k + 1).astype(F32).T
        dst_ref[at(0, 6 + k), :] = jnp.where(r_i > c_i, one, jnp.where(r_i < c_i, two, 0.0)).astype(BF16)
    parts = [[], [], []]
    for k in range(N // NB):
        rest = scale_ref[k * NB : (k + 1) * NB, :].T[0:1, :]
        for part in parts:
            part.append(rest)
            rest = rest - rest.astype(BF16).astype(F32)
    dst_ref[TAIL:PACKED, :] = pick_rows(sum(parts, [])).astype(BF16)


def unpack_unit(src_ref, e_ref, scale_ref, row_ref):
    r_i, c_i = iotas()
    eye = jnp.where(r_i == c_i, 1.0, 0.0)
    zero = jnp.zeros((NB, NB), BF16)
    for b, (r, c) in enumerate(LOWER):
        e_ref[r * NB : (r + 1) * NB, c * NB : (c + 1) * NB] = src_ref[at(0, b), :]
        e_ref[c * NB : (c + 1) * NB, r * NB : (r + 1) * NB] = zero
    for k in range(2):
        pair = src_ref[at(0, 6 + k), :].astype(F32)
        for d, value in ((2 * k, pair), (2 * k + 1, pair.T)):
            e_ref[d * NB : (d + 1) * NB, d * NB : (d + 1) * NB] = jnp.where(r_i > c_i, value, eye).astype(BF16)
    tile = src_ref[TAIL:PACKED, :].astype(F32)
    for k in range(N // NB):
        row = tile[k : k + 1, :] + tile[4 + k : 5 + k, :] + tile[8 + k : 9 + k, :]
        row_ref[:, k * NB : (k + 1) * NB] = jnp.broadcast_to(row, (8, NB))
        scale_ref[k * NB : (k + 1) * NB, :] = jnp.broadcast_to(row, (NB, NB)).T


def scale_row(scale_ref, row_ref):
    for k in range(N // NB):
        row_ref[:, k * NB : (k + 1) * NB] = scale_ref[k * NB : (k + 1) * NB, :].T[0:8, :]


def pack_symmetric(value, dst_ref):
    r_i, c_i = iotas()
    for b, (r, c) in enumerate(LOWER):
        dst_ref[at(0, b), :] = block(value, r, c).astype(BF16)
    rows = []
    for k in range(2):
        two = block(value, 2 * k + 1, 2 * k + 1)
        dst_ref[at(0, 6 + k), :] = jnp.where(r_i >= c_i, block(value, 2 * k, 2 * k), two).astype(BF16)
        rows.append(jnp.sum(jnp.where(r_i == c_i, two, 0.0), 0, keepdims=True))
    dst_ref[TAIL:PACKED, :] = pick_rows(rows).astype(BF16)


def add_symmetric(src_ref, dst_ref):
    r_i, c_i = iotas()

    def sub(r, c, value):
        rows, cols = slice(r * NB, (r + 1) * NB), slice(c * NB, (c + 1) * NB)
        dst_ref[rows, cols] = dst_ref[rows, cols] - value

    for b, (r, c) in enumerate(LOWER):
        value = src_ref[at(0, b), :].astype(F32)
        sub(r, c, value)
        sub(c, r, value.T)
    tile = src_ref[TAIL:PACKED, :].astype(F32)
    for k in range(2):
        pair = src_ref[at(0, 6 + k), :].astype(F32)
        turned = pair.T
        sub(2 * k, 2 * k, jnp.where(r_i >= c_i, pair, turned))
        diagonal = jnp.broadcast_to(tile[k : k + 1, :], (NB, NB))
        two = jnp.where(r_i < c_i, pair, turned)
        sub(2 * k + 1, 2 * k + 1, jnp.where(r_i == c_i, diagonal, two))


def solve_t(e_ref, row_ref, c_ref, out_ref):
    h = N // 2
    row = row_ref[0:1, :]
    out_ref[:, 0:h] = (dot(c_ref[:, 0:h], e_ref[0:h, 0:h], 1, 1) * row[:, 0:h]).astype(BF16)
    out_ref[:, h:N] = (dot(c_ref[...], e_ref[h:N, :], 1, 1) * row[:, h:N]).astype(BF16)


def solve_n(e_ref, scale_ref, c_ref, out_ref):
    h = N // 2
    out_ref[0:h, :] = (dot(e_ref[0:h, 0:h], c_ref[0:h, :]) * tiled(scale_ref[0:h, :])).astype(BF16)
    out_ref[h:N, :] = (dot(e_ref[h:N, :], c_ref[...]) * tiled(scale_ref[h:N, :])).astype(BF16)


ANY = pl.BlockSpec(memory_space=pl.ANY)
VM = pl.BlockSpec(memory_space=pltpu.VMEM)
B16 = pltpu.VMEM((N, N), BF16)
WIDE = pltpu.VMEM((N, N), F32)


def shape(dims, kind):
    return jax.ShapeDtypeStruct(dims, kind)


def call(kernel, outs, in_specs, out_specs, scratch, flops, limit, aliases=None):
    return pl.pallas_call(
        kernel,
        out_shape=outs,
        in_specs=in_specs,
        out_specs=out_specs,
        scratch_shapes=scratch,
        input_output_aliases=aliases or {},
        compiler_params=pltpu.CompilerParams(vmem_limit_bytes=limit << 20),
        cost_estimate=pl.CostEstimate(flops=flops * 10**9, bytes_accessed=4 << 20, transcendentals=0),
    )


WORK = [pltpu.VMEM((NB, 2 * NB), F32)] * 6 + [pltpu.VMEM((NB, N), F32)] * 2 + [WIDE] * 4
DMA2 = pltpu.SemaphoreType.DMA((2,))
ENDS = (shape((N, N), BF16), shape((N, N), BF16), shape((N, NB), F32), shape((N, NB), F32))


def factor_part(first, last):
    lo, hi = first * NB, last * NB
    ending = hi == N

    def kernel(*refs):
        refs = list(refs)
        take = lambda n: [refs.pop(0) for _ in range(n)]
        source = take(1)[0]
        before = take(6) if first else ()
        l_out = take(1)[0]
        after = take(5) if ending else take(6)
        x0, x1, p0, p1, s0, s1, w0, w1, g0, g1, l0, l1 = take(12)
        state = tuple(after[:4]) if ending else tuple(take(4))
        in_sem, out_sem = take(2)
        if first:
            for dst, src in zip((g0, g1), before):
                dst[lo:N, :] = src[...]
            for dst, src in zip(state, before[2:]):
                dst[0:lo, :] = src[...]
        else:
            copies = [
                pltpu.make_async_copy(source.at[m, m], g_ref, in_sem.at[m])
                for m, g_ref in enumerate((g0, g1))
            ]
            for c in copies:
                c.start()
            for c in copies:
                c.wait()
        factor_steps(first, last, (g0, g1), (x0, x1), (p0, p1), (s0, s1), (w0, w1), (l0, l1), state[:2], state[2:])
        outs = [
            pltpu.make_async_copy(l_ref.at[:, lo:hi], l_out.at[m, 0, :, lo:hi], out_sem.at[m])
            for m, l_ref in enumerate((l0, l1))
        ]
        for c in outs:
            c.start()
        if ending:
            pack_unit(state[0], state[2], after[4])
        else:
            for dst, src in zip(after, (g0, g1)):
                dst[...] = src[hi:N, :]
            for dst, src in zip(after[2:], state):
                dst[...] = src[0:hi, :]
        for c in outs:
            c.wait()

    if ending:
        outs = ENDS + (shape((PACKED, NB), BF16),)
        scratch = []
    else:
        outs = (shape((N - hi, N), F32),) * 2 + (shape((hi, N), BF16),) * 2 + (shape((hi, NB), F32),) * 2
        scratch = [B16, B16, pltpu.VMEM((N, NB), F32), pltpu.VMEM((N, NB), F32)]
    return call(
        kernel, (shape((2, 1, N, N), F32),) + outs,
        [ANY] + [VM] * (6 if first else 0), (ANY,) + (VM,) * len(outs),
        WORK + scratch + [DMA2, DMA2], 15 * (last - first), 13, {0: 0} if first else None,
    )


def products_kernel(h_ref, v_ref, e1, scale1, to_right, to_below, y2, y3, c2, c3, in_sem):
    copies = [
        pltpu.make_async_copy(h_ref.at[1, 1], c2, in_sem.at[0]),
        pltpu.make_async_copy(v_ref.at[1, 1], c3, in_sem.at[1]),
    ]
    for c in copies:
        c.start()
    for c in copies:
        c.wait()
    solve_n(e1, scale1, c2, y2)
    solve_n(e1, scale1, c3, y3)
    t2 = y2[...].T
    pack_symmetric(dot(t2, y2[...]), to_right)
    side = dot(t2, y3[...])
    for r in range(N // NB):
        for c in range(N // NB):
            to_right[at(PACKED, 4 * r + c), :] = block(side, r, c).astype(BF16)
    pack_symmetric(dot(y3[...].T, y3[...]), to_below)


def products_call(*args):
    return call(
        products_kernel,
        (shape((PACKED + N * N // NB, NB), BF16), shape((PACKED, NB), BF16), shape((N, N), BF16),
         shape((N, N), BF16)),
        [ANY] * 2 + [VM] * 2, (VM,) * 4, [B16, B16, DMA2], 4, 8,
    )(*args)


def local_kernel(d_ref, h_ref, v_ref, e0, e1, scale0, scale1, y2, y3, sbuf, dbuf, link_out,
                 c0, c1, f2, f3, y0, y1, z2, z3, lbuf, row1, in_sem, out_sem):
    copies = [
        pltpu.make_async_copy(src, dst, in_sem.at[k])
        for k, (src, dst) in enumerate(
            (
                (h_ref.at[1, 0], c0),
                (v_ref.at[0, 1], c1),
                (h_ref.at[0, 0], f2),
                (v_ref.at[0, 0], f3),
                (d_ref.at[0, 1], sbuf.at[0]),
                (d_ref.at[1, 0], sbuf.at[1]),
            )
        )
    ]
    for c in copies:
        c.start()
    scale_row(scale1, row1)
    for c in copies[:4]:
        c.wait()
    outs = []
    solve_t(e1, row1, c1, y1)
    put_link(outs, lbuf, link_out, out_sem, 0, 1, dot(y1[...], y3[...]))
    solve_t(e1, row1, c0, y0)
    put_link(outs, lbuf, link_out, out_sem, 1, 0, dot(y0[...], y2[...]))
    solve_n(e0, scale0, f2, z2)
    solve_n(e0, scale0, f3, z3)
    u2 = z2[...].T
    put_link(outs, lbuf, link_out, out_sem, 0, 3, dot(u2, z3[...]) + dot(y1[...], y0[...], 1, 1))
    dbuf[0] = dot(y1[...], y2[...])
    dbuf[1] = dot(y0[...], y3[...])
    for c in copies[4:]:
        c.wait()
    sbuf[0] = sbuf[0] - (dot(u2, z2[...]) + dot(y1[...], y1[...], 1, 1))
    sbuf[1] = sbuf[1] - (dot(z3[...].T, z3[...]) + dot(y0[...], y0[...], 1, 1))
    for c in outs:
        c.wait()


def local_call(*args):
    return call(
        local_kernel,
        (shape((2, N, N), F32), shape((2, N, N), F32), shape((2, 1, 4, N, N), BF16)),
        [ANY] * 3 + [VM] * 6, (VM, VM, ANY),
        [B16] * 8 + [pltpu.VMEM((3, N, N), BF16), pltpu.VMEM((8, N), F32)]
        + [pltpu.SemaphoreType.DMA((6,)), pltpu.SemaphoreType.DMA((3,))],
        9, 16,
    )(*args)


def put_link(outs, buffer, out, sem, row, which, value):
    slot = len(outs)
    buffer[slot] = (-value).astype(BF16)
    copy = pltpu.make_async_copy(buffer.at[slot], out.at[row, 0, which], sem.at[slot])
    copy.start()
    outs.append(copy)


def right_kernel(h_ref, rpack, rc, se, schur_in, link_in, schur0, link_out,
                 inv, c0, w0, w2, w3, scale, row, lbuf, in_sem, sem):
    load = pltpu.make_async_copy(h_ref.at[0, 1], c0, in_sem)
    load.start()
    unpack_unit(rpack, inv, scale, row)
    load.wait()
    outs = []
    solve_t(inv, row, c0, w0)
    solve_n(inv, scale, rc.at[0], w2)
    put_link(outs, lbuf, link_out, sem, 0, 0, dot(w0[...], w2[...]))
    solve_n(inv, scale, rc.at[1], w3)
    put_link(outs, lbuf, link_out, sem, 0, 2, dot(w0[...], w3[...]) + se[0])
    schur0[...] = schur_in[0] - dot(w0[...], w0[...], 1, 1)
    for c in outs:
        c.wait()


def right_call(*args):
    return call(
        right_kernel, (shape((N, N), F32), shape((2, 1, 4, N, N), BF16)),
        [ANY] + [VM] * 4 + [ANY], (VM, ANY),
        [B16] * 5 + [pltpu.VMEM((N, NB), F32), pltpu.VMEM((8, N), F32), pltpu.VMEM((2, N, N), BF16)]
        + [pltpu.SemaphoreType.DMA, DMA2],
        5, 10, {5: 1},
    )(*args)


def sides_kernel(from_left, from_above, schur0, schur_in, schur_out, schur1, sbuf, sem):
    sbuf[...] = schur0[...]
    add_symmetric(from_above, sbuf)
    copy = pltpu.make_async_copy(sbuf, schur_out.at[0, 0], sem)
    copy.start()
    schur1[...] = schur_in[1]
    add_symmetric(from_left, schur1)
    copy.wait()


def sides_call(*args):
    return call(
        sides_kernel, (shape((2, 1, N, N), F32), shape((N, N), F32)),
        [VM] * 4, (ANY, VM), [WIDE, pltpu.SemaphoreType.DMA], 1, 6,
    )(*args)


def below_kernel(v_ref, bpack, bc, bc0, se, from_left, schur1, schur_in, link_in, schur_out, link_out,
                 inv, c1, w0, w1, w2, w3, scale, row, lbuf, sbuf, in_sem, sem):
    load = pltpu.make_async_copy(v_ref.at[1, 0], c1, in_sem)
    load.start()
    unpack_unit(bpack, inv, scale, row)
    load.wait()
    outs = []
    solve_t(inv, row, c1, w1)
    sbuf[...] = schur1[...] - dot(w1[...], w1[...], 1, 1)
    copy = pltpu.make_async_copy(sbuf, schur_out.at[1, 0], sem.at[3])
    copy.start()
    solve_n(inv, scale, bc.at[1], w3)
    put_link(outs, lbuf, link_out, sem, 1, 1, dot(w1[...], w3[...]))
    solve_n(inv, scale, bc.at[0], w2)
    put_link(outs, lbuf, link_out, sem, 1, 2, dot(w1[...], w2[...]) + se[1])
    solve_t(inv, row, bc0, w0)
    side = jnp.concatenate(
        [
            jnp.concatenate([from_left[at(PACKED, 4 * r + c), :] for c in range(N // NB)], 1)
            for r in range(N // NB)
        ],
        0,
    )
    put_link(outs, lbuf, link_out, sem, 1, 3, dot(w1[...], w0[...], 1, 1) + side.astype(F32))
    for c in outs + [copy]:
        c.wait()


def below_call(*args):
    return call(
        below_kernel, (shape((2, 1, N, N), F32), shape((2, 1, 4, N, N), BF16)),
        [ANY] + [VM] * 6 + [ANY, ANY], (ANY, ANY),
        [B16] * 6 + [pltpu.VMEM((N, NB), F32), pltpu.VMEM((8, N), F32), pltpu.VMEM((3, N, N), BF16), WIDE]
        + [pltpu.SemaphoreType.DMA, pltpu.SemaphoreType.DMA((4,))],
        6, 12, {7: 0, 8: 1},
    )(*args)


def passed(value, down, right):
    rows, cols = lax.axis_size("row"), lax.axis_size("col")
    pairs = [
        (r * cols + c, ((r + down) % rows) * cols + (c + right) % cols)
        for r in range(rows)
        for c in range(cols)
    ]
    return lax.ppermute(value, ("row", "col"), pairs)


def on_device(diag_blocks, horizontal, vertical):
    pair = jnp.stack([horizontal[0, 0], vertical[0, 0]])
    right = passed(pair, 0, -1)
    below0 = passed(horizontal[0, 1], -1, 1)
    state = factor_part(0, 2)(diag_blocks)
    below = passed(right, -1, 1)
    factor, e0, e1, scale0, scale1, packed = factor_part(2, 4)(*state)
    right_inverse = passed(packed, 0, -1)
    to_right, to_below, y2, y3 = products_call(horizontal, vertical, e1, scale1)
    from_left = passed(to_right, 0, 1)
    from_above = passed(to_below, 1, 0)
    below_inverse = passed(right_inverse, -1, 1)
    schur, southeast, links = local_call(
        diag_blocks, horizontal, vertical, e0, e1, scale0, scale1, y2, y3
    )
    schur0, links = right_call(horizontal, right_inverse, right, southeast, schur, links)
    schur, schur1 = sides_call(from_left, from_above, schur0, schur)
    schur, links = below_call(vertical, below_inverse, below, below0, southeast, from_left, schur1, schur, links)
    return (factor, schur, links)


def solution(mesh):
    blocks = P("row", "col", None, None)
    return jax.shard_map(
        on_device,
        mesh=mesh,
        in_specs=(blocks, blocks, blocks),
        out_specs=(blocks, blocks, P("row", "col", None, None, None)),
        check_vma=False,
    )
```

```python
import jax
import jax.numpy as jnp
from jax import lax
from jax.experimental import pallas as pl
from jax.experimental.pallas import tpu as pltpu
from jax.sharding import PartitionSpec as P

N = 512
NB = 128
SB = 16
F32 = jnp.float32
BF16 = jnp.bfloat16


def dot(a, b, ca=1, cb=0):
    return lax.dot_general(a, b, (((ca,), (cb,)), ((), ())), preferred_element_type=F32)


def split(x):
    hi = x.astype(BF16)
    return hi, (x - hi.astype(F32)).astype(BF16)


def dot3(a, b, cb=0):
    ah, al = a
    bh, bl = b
    if cb == 1:
        return dot(ah, bh, 1, 1) + dot(al, bh, 1, 1) + dot(ah, bl, 1, 1)
    return dot(jnp.concatenate([ah, al], 1), jnp.concatenate([bh, bh], 0)) + dot(ah, bl)


def rows8(x, k):
    return jnp.broadcast_to(x[k : k + 1, :], (8, NB))


def eliminate(s, x_ref, p_ref, s_ref):
    k0 = SB * s
    row = lax.broadcasted_iota(jnp.int32, (8, NB), 0)
    xs = [[x_ref[k0 + 8 * h : k0 + 8 * h + 8, NB * w : NB * w + NB] for h in range(2)] for w in range(2)]
    cols = [
        [jnp.broadcast_to(xs[0][h][:, k0 + c : k0 + c + 1], (8, NB)) for h in range(2)]
        for c in range(SB)
    ]
    pivots = [jnp.ones((8, NB), F32) for _ in range(2)]
    inverses = [jnp.ones((8, NB), F32) for _ in range(2)]
    saved = [[xs[w][h] for h in range(2)] for w in range(2)]
    for k in range(SB):
        kh, kr = divmod(k, 8)
        is_k = row == kr
        pivot = rows8(cols[k][kh], kr)
        inverse = 1.0 / pivot
        mult = [cols[k][h] * inverse for h in range(2)]
        mult[kh] = jnp.where(is_k, 0.0, mult[kh])
        for c in range(k + 1, SB):
            head = rows8(cols[c][kh], kr)
            cols[c] = [cols[c][h] - mult[h] * head for h in range(2)]
        pivots[kh] = jnp.where(is_k, pivot, pivots[kh])
        inverses[kh] = jnp.where(is_k, inverse, inverses[kh])
        for w in range(2):
            saved[w][kh] = jnp.where(is_k, xs[w][kh], saved[w][kh])
            head = rows8(xs[w][kh], kr)
            xs[w] = [xs[w][h] - mult[h] * head for h in range(2)]
    for h in range(2):
        scale = lax.rsqrt(pivots[h])
        s_ref[k0 + 8 * h : k0 + 8 * h + 8, 0:NB] = scale
        s_ref[k0 + 8 * h : k0 + 8 * h + 8, NB : 2 * NB] = pivots[h] * scale
        for w in range(2):
            p_ref[k0 + 8 * h : k0 + 8 * h + 8, NB * w : NB * w + NB] = saved[w][h] * scale
    below = NB - k0 - SB
    if below:
        z = jnp.concatenate(
            [jnp.concatenate([xs[w][h] * inverses[h] for w in range(2)], 1) for h in range(2)], 0
        )
        zh, zl = split(z)

        def pad(v):
            parts = [v]
            if k0:
                parts.insert(0, jnp.zeros((k0, 2 * NB), BF16))
            parts.append(jnp.zeros((below, 2 * NB), BF16))
            return jnp.concatenate(parts, 0)

        a = split(x_ref[k0 + SB : NB, 0:NB])
        x_ref[k0 + SB : NB, :] = x_ref[k0 + SB : NB, :] - dot3(a, (pad(zh), pad(zl)))


def tiled(x):
    return jnp.concatenate([x] * (N // NB), 1)


def factor_steps(first, last, g_refs, x_refs, p_refs, s_refs, w_refs, l_refs, e_refs, scale_refs):
    r_i = lax.broadcasted_iota(jnp.int32, (NB, NB), 0)
    c_i = lax.broadcasted_iota(jnp.int32, (NB, NB), 1)
    wide = lax.broadcasted_iota(jnp.int32, (NB, N), 1)
    for l_ref in l_refs:
        for c in range(first, last):
            if c:
                l_ref[0 : c * NB, c * NB : (c + 1) * NB] = jnp.zeros((c * NB, NB), F32)

    def outer(o, carry):
        base = pl.multiple_of(o * NB, NB)
        here = pl.ds(base, NB)
        for g_ref, x_ref in zip(g_refs, x_refs):
            x_ref[:, 0:NB] = g_ref[here, here]
            x_ref[:, NB : 2 * NB] = jnp.where(r_i == c_i, 1.0, 0.0)
        for s in range(NB // SB):
            for x_ref, p_ref, s_ref in zip(x_refs, p_refs, s_refs):
                eliminate(s, x_ref, p_ref, s_ref)
        for m in range(2):
            p_ref, s_ref, w_ref = p_refs[m], s_refs[m], w_refs[m]
            l_refs[m][here, here] = jnp.where(r_i >= c_i, p_ref[:, 0:NB].T, 0.0)
            inverse = p_ref[:, NB : 2 * NB]
            w_ref[...] = dot3(split(inverse), split(g_refs[m][here, :]))
            w_ref[:, here] = inverse
            unit = w_ref[...] * tiled(s_ref[:, NB : 2 * NB])
            e_refs[m][here, :] = jnp.where(wide < base + NB, unit, 0.0).astype(BF16)
            scale_refs[m][here, :] = s_ref[:, 0:NB]
        for p in range(first + 1, N // NB):
            rows = slice(p * NB, (p + 1) * NB)

            @pl.when(p > o)
            def _():
                for g_ref, p_ref, w_ref, l_ref in zip(g_refs, p_refs, w_refs, l_refs):
                    lower = dot3(split(g_ref[rows, here]), split(p_ref[:, NB : 2 * NB]), 1)
                    l_ref[rows, here] = lower
                    g_ref[rows, here] = jnp.zeros((NB, NB), F32)
                    g_ref[rows, :] = g_ref[rows, :] - dot3(split(lower), split(w_ref[...]))

        return carry

    lax.fori_loop(first, last, outer, 0)


LOWER = [(r, c) for r in range(N // NB) for c in range(r)]
TAIL = 8 * NB
PACKED = TAIL + SB


def block(ref, r, c):
    return ref[r * NB : (r + 1) * NB, c * NB : (c + 1) * NB]


def at(first, b):
    return slice(first + b * NB, first + (b + 1) * NB)


def iotas():
    return (
        lax.broadcasted_iota(jnp.int32, (NB, NB), 0),
        lax.broadcasted_iota(jnp.int32, (NB, NB), 1),
    )


def pick_rows(rows):
    where = lax.broadcasted_iota(jnp.int32, (SB, NB), 0)
    tile = jnp.zeros((SB, NB), F32)
    for k, row in enumerate(rows):
        tile = jnp.where(where == k, jnp.broadcast_to(row, (SB, NB)), tile)
    return tile


def pack_unit(e_ref, scale_ref, dst_ref):
    r_i, c_i = iotas()
    for b, (r, c) in enumerate(LOWER):
        dst_ref[at(0, b), :] = block(e_ref, r, c)
    for k in range(2):
        one = block(e_ref, 2 * k, 2 * k).astype(F32)
        two = block(e_ref, 2 * k + 1, 2 * k + 1).astype(F32).T
        dst_ref[at(0, 6 + k), :] = jnp.where(r_i > c_i, one, jnp.where(r_i < c_i, two, 0.0)).astype(BF16)
    parts = [[], [], []]
    for k in range(N // NB):
        rest = scale_ref[k * NB : (k + 1) * NB, :].T[0:1, :]
        for part in parts:
            part.append(rest)
            rest = rest - rest.astype(BF16).astype(F32)
    dst_ref[TAIL:PACKED, :] = pick_rows(sum(parts, [])).astype(BF16)


def unpack_unit(src_ref, e_ref, scale_ref, row_ref):
    r_i, c_i = iotas()
    eye = jnp.where(r_i == c_i, 1.0, 0.0)
    zero = jnp.zeros((NB, NB), BF16)
    for b, (r, c) in enumerate(LOWER):
        e_ref[r * NB : (r + 1) * NB, c * NB : (c + 1) * NB] = src_ref[at(0, b), :]
        e_ref[c * NB : (c + 1) * NB, r * NB : (r + 1) * NB] = zero
    for k in range(2):
        pair = src_ref[at(0, 6 + k), :].astype(F32)
        for d, value in ((2 * k, pair), (2 * k + 1, pair.T)):
            e_ref[d * NB : (d + 1) * NB, d * NB : (d + 1) * NB] = jnp.where(r_i > c_i, value, eye).astype(BF16)
    tile = src_ref[TAIL:PACKED, :].astype(F32)
    for k in range(N // NB):
        row = tile[k : k + 1, :] + tile[4 + k : 5 + k, :] + tile[8 + k : 9 + k, :]
        row_ref[:, k * NB : (k + 1) * NB] = jnp.broadcast_to(row, (8, NB))
        scale_ref[k * NB : (k + 1) * NB, :] = jnp.broadcast_to(row, (NB, NB)).T


def scale_row(scale_ref, row_ref):
    for k in range(N // NB):
        row_ref[:, k * NB : (k + 1) * NB] = scale_ref[k * NB : (k + 1) * NB, :].T[0:8, :]


def pack_symmetric(value, dst_ref):
    r_i, c_i = iotas()
    for b, (r, c) in enumerate(LOWER):
        dst_ref[at(0, b), :] = block(value, r, c).astype(BF16)
    rows = []
    for k in range(2):
        two = block(value, 2 * k + 1, 2 * k + 1)
        dst_ref[at(0, 6 + k), :] = jnp.where(r_i >= c_i, block(value, 2 * k, 2 * k), two).astype(BF16)
        rows.append(jnp.sum(jnp.where(r_i == c_i, two, 0.0), 0, keepdims=True))
    dst_ref[TAIL:PACKED, :] = pick_rows(rows).astype(BF16)


def add_symmetric(src_ref, dst_ref):
    r_i, c_i = iotas()

    def sub(r, c, value):
        rows, cols = slice(r * NB, (r + 1) * NB), slice(c * NB, (c + 1) * NB)
        dst_ref[rows, cols] = dst_ref[rows, cols] - value

    for b, (r, c) in enumerate(LOWER):
        value = src_ref[at(0, b), :].astype(F32)
        sub(r, c, value)
        sub(c, r, value.T)
    tile = src_ref[TAIL:PACKED, :].astype(F32)
    for k in range(2):
        pair = src_ref[at(0, 6 + k), :].astype(F32)
        turned = pair.T
        sub(2 * k, 2 * k, jnp.where(r_i >= c_i, pair, turned))
        diagonal = jnp.broadcast_to(tile[k : k + 1, :], (NB, NB))
        two = jnp.where(r_i < c_i, pair, turned)
        sub(2 * k + 1, 2 * k + 1, jnp.where(r_i == c_i, diagonal, two))


def solve_t(e_ref, row_ref, c_ref, out_ref):
    h = N // 2
    row = row_ref[0:1, :]
    out_ref[:, 0:h] = (dot(c_ref[:, 0:h], e_ref[0:h, 0:h], 1, 1) * row[:, 0:h]).astype(BF16)
    out_ref[:, h:N] = (dot(c_ref[...], e_ref[h:N, :], 1, 1) * row[:, h:N]).astype(BF16)


def solve_n(e_ref, scale_ref, c_ref, out_ref):
    h = N // 2
    out_ref[0:h, :] = (dot(e_ref[0:h, 0:h], c_ref[0:h, :]) * tiled(scale_ref[0:h, :])).astype(BF16)
    out_ref[h:N, :] = (dot(e_ref[h:N, :], c_ref[...]) * tiled(scale_ref[h:N, :])).astype(BF16)


ANY = pl.BlockSpec(memory_space=pl.ANY)
VM = pl.BlockSpec(memory_space=pltpu.VMEM)
B16 = pltpu.VMEM((N, N), BF16)
WIDE = pltpu.VMEM((N, N), F32)


def shape(dims, kind):
    return jax.ShapeDtypeStruct(dims, kind)


def call(kernel, outs, in_specs, out_specs, scratch, flops, limit, aliases=None):
    return pl.pallas_call(
        kernel,
        out_shape=outs,
        in_specs=in_specs,
        out_specs=out_specs,
        scratch_shapes=scratch,
        input_output_aliases=aliases or {},
        compiler_params=pltpu.CompilerParams(vmem_limit_bytes=limit << 20),
        cost_estimate=pl.CostEstimate(flops=flops * 10**9, bytes_accessed=4 << 20, transcendentals=0),
    )


WORK = [pltpu.VMEM((NB, 2 * NB), F32)] * 6 + [pltpu.VMEM((NB, N), F32)] * 2 + [WIDE] * 4
DMA2 = pltpu.SemaphoreType.DMA((2,))
ENDS = (shape((N, N), BF16), shape((N, N), BF16), shape((N, NB), F32), shape((N, NB), F32))


def factor_part(first, last):
    lo, hi = first * NB, last * NB
    ending = hi == N

    def kernel(*refs):
        refs = list(refs)
        take = lambda n: [refs.pop(0) for _ in range(n)]
        source = take(1)[0]
        before = take(6) if first else ()
        l_out = take(1)[0]
        after = take(5) if ending else take(6)
        x0, x1, p0, p1, s0, s1, w0, w1, g0, g1, l0, l1 = take(12)
        state = tuple(after[:4]) if ending else tuple(take(4))
        in_sem, out_sem = take(2)
        if first:
            for dst, src in zip((g0, g1), before):
                dst[lo:N, :] = src[...]
            for dst, src in zip(state, before[2:]):
                dst[0:lo, :] = src[...]
        else:
            copies = [
                pltpu.make_async_copy(source.at[m, m], g_ref, in_sem.at[m])
                for m, g_ref in enumerate((g0, g1))
            ]
            for c in copies:
                c.start()
            for c in copies:
                c.wait()
        factor_steps(first, last, (g0, g1), (x0, x1), (p0, p1), (s0, s1), (w0, w1), (l0, l1), state[:2], state[2:])
        outs = [
            pltpu.make_async_copy(l_ref.at[:, lo:hi], l_out.at[m, 0, :, lo:hi], out_sem.at[m])
            for m, l_ref in enumerate((l0, l1))
        ]
        for c in outs:
            c.start()
        if ending:
            pack_unit(state[0], state[2], after[4])
        else:
            for dst, src in zip(after, (g0, g1)):
                dst[...] = src[hi:N, :]
            for dst, src in zip(after[2:], state):
                dst[...] = src[0:hi, :]
        for c in outs:
            c.wait()

    if ending:
        outs = ENDS + (shape((PACKED, NB), BF16),)
        scratch = []
    else:
        outs = (shape((N - hi, N), F32),) * 2 + (shape((hi, N), BF16),) * 2 + (shape((hi, NB), F32),) * 2
        scratch = [B16, B16, pltpu.VMEM((N, NB), F32), pltpu.VMEM((N, NB), F32)]
    return call(
        kernel, (shape((2, 1, N, N), F32),) + outs,
        [ANY] + [VM] * (6 if first else 0), (ANY,) + (VM,) * len(outs),
        WORK + scratch + [DMA2, DMA2], 15 * (last - first), 13, {0: 0} if first else None,
    )


def products_kernel(h_ref, v_ref, e1, scale1, to_right, to_below, y2, y3, c2, c3, in_sem):
    copies = [
        pltpu.make_async_copy(h_ref.at[1, 1], c2, in_sem.at[0]),
        pltpu.make_async_copy(v_ref.at[1, 1], c3, in_sem.at[1]),
    ]
    for c in copies:
        c.start()
    for c in copies:
        c.wait()
    solve_n(e1, scale1, c2, y2)
    solve_n(e1, scale1, c3, y3)
    t2 = y2[...].T
    pack_symmetric(dot(t2, y2[...]), to_right)
    side = dot(t2, y3[...])
    for r in range(N // NB):
        for c in range(N // NB):
            to_right[at(PACKED, 4 * r + c), :] = block(side, r, c).astype(BF16)
    pack_symmetric(dot(y3[...].T, y3[...]), to_below)


def products_call(*args):
    return call(
        products_kernel,
        (shape((PACKED + N * N // NB, NB), BF16), shape((PACKED, NB), BF16), shape((N, N), BF16),
         shape((N, N), BF16)),
        [ANY] * 2 + [VM] * 2, (VM,) * 4, [B16, B16, DMA2], 4, 8,
    )(*args)


def local_kernel(d_ref, h_ref, v_ref, e0, e1, scale0, scale1, y2, y3, sbuf, dbuf, link_out,
                 c0, c1, f2, f3, y0, y1, z2, z3, lbuf, row1, in_sem, out_sem):
    copies = [
        pltpu.make_async_copy(src, dst, in_sem.at[k])
        for k, (src, dst) in enumerate(
            (
                (h_ref.at[1, 0], c0),
                (v_ref.at[0, 1], c1),
                (h_ref.at[0, 0], f2),
                (v_ref.at[0, 0], f3),
                (d_ref.at[0, 1], sbuf.at[0]),
                (d_ref.at[1, 0], sbuf.at[1]),
            )
        )
    ]
    for c in copies:
        c.start()
    scale_row(scale1, row1)
    for c in copies[:4]:
        c.wait()
    outs = []
    solve_t(e1, row1, c1, y1)
    put_link(outs, lbuf, link_out, out_sem, 0, 1, dot(y1[...], y3[...]))
    solve_t(e1, row1, c0, y0)
    put_link(outs, lbuf, link_out, out_sem, 1, 0, dot(y0[...], y2[...]))
    solve_n(e0, scale0, f2, z2)
    solve_n(e0, scale0, f3, z3)
    u2 = z2[...].T
    put_link(outs, lbuf, link_out, out_sem, 0, 3, dot(u2, z3[...]) + dot(y1[...], y0[...], 1, 1))
    dbuf[0] = dot(y1[...], y2[...])
    dbuf[1] = dot(y0[...], y3[...])
    for c in copies[4:]:
        c.wait()
    sbuf[0] = sbuf[0] - (dot(u2, z2[...]) + dot(y1[...], y1[...], 1, 1))
    sbuf[1] = sbuf[1] - (dot(z3[...].T, z3[...]) + dot(y0[...], y0[...], 1, 1))
    for c in outs:
        c.wait()


def local_call(*args):
    return call(
        local_kernel,
        (shape((2, N, N), F32), shape((2, N, N), F32), shape((2, 1, 4, N, N), BF16)),
        [ANY] * 3 + [VM] * 6, (VM, VM, ANY),
        [B16] * 8 + [pltpu.VMEM((3, N, N), BF16), pltpu.VMEM((8, N), F32)]
        + [pltpu.SemaphoreType.DMA((6,)), pltpu.SemaphoreType.DMA((3,))],
        9, 16,
    )(*args)


def put_link(outs, buffer, out, sem, row, which, value):
    slot = len(outs)
    buffer[slot] = (-value).astype(BF16)
    copy = pltpu.make_async_copy(buffer.at[slot], out.at[row, 0, which], sem.at[slot])
    copy.start()
    outs.append(copy)


def right_kernel(h_ref, rpack, rc, se, schur_in, link_in, schur0, link_out,
                 inv, c0, w0, w2, w3, scale, row, lbuf, in_sem, sem):
    load = pltpu.make_async_copy(h_ref.at[0, 1], c0, in_sem)
    load.start()
    unpack_unit(rpack, inv, scale, row)
    load.wait()
    outs = []
    solve_t(inv, row, c0, w0)
    solve_n(inv, scale, rc.at[0], w2)
    put_link(outs, lbuf, link_out, sem, 0, 0, dot(w0[...], w2[...]))
    solve_n(inv, scale, rc.at[1], w3)
    put_link(outs, lbuf, link_out, sem, 0, 2, dot(w0[...], w3[...]) + se[0])
    schur0[...] = schur_in[0] - dot(w0[...], w0[...], 1, 1)
    for c in outs:
        c.wait()


def right_call(*args):
    return call(
        right_kernel, (shape((N, N), F32), shape((2, 1, 4, N, N), BF16)),
        [ANY] + [VM] * 4 + [ANY], (VM, ANY),
        [B16] * 5 + [pltpu.VMEM((N, NB), F32), pltpu.VMEM((8, N), F32), pltpu.VMEM((2, N, N), BF16)]
        + [pltpu.SemaphoreType.DMA, DMA2],
        5, 10, {5: 1},
    )(*args)


def below_kernel(v_ref, bpack, bc, bc0, se, from_left, from_above, schur0, schur_in, link_in, schur_out, link_out,
                 inv, c1, w0, w1, w2, w3, scale, row, lbuf, sbuf, in_sem, sem):
    load = pltpu.make_async_copy(v_ref.at[1, 0], c1, in_sem)
    load.start()
    unpack_unit(bpack, inv, scale, row)
    sbuf[0] = schur0[...]
    add_symmetric(from_above, sbuf.at[0])
    stores = [pltpu.make_async_copy(sbuf.at[m], schur_out.at[m, 0], sem.at[3 + m]) for m in range(2)]
    stores[0].start()
    load.wait()
    outs = []
    solve_t(inv, row, c1, w1)
    sbuf[1] = schur_in[1] - dot(w1[...], w1[...], 1, 1)
    add_symmetric(from_left, sbuf.at[1])
    stores[1].start()
    solve_n(inv, scale, bc.at[1], w3)
    put_link(outs, lbuf, link_out, sem, 1, 1, dot(w1[...], w3[...]))
    solve_n(inv, scale, bc.at[0], w2)
    put_link(outs, lbuf, link_out, sem, 1, 2, dot(w1[...], w2[...]) + se[1])
    solve_t(inv, row, bc0, w0)
    side = jnp.concatenate(
        [
            jnp.concatenate([from_left[at(PACKED, 4 * r + c), :] for c in range(N // NB)], 1)
            for r in range(N // NB)
        ],
        0,
    )
    put_link(outs, lbuf, link_out, sem, 1, 3, dot(w1[...], w0[...], 1, 1) + side.astype(F32))
    for c in outs + stores:
        c.wait()


def below_call(*args):
    return call(
        below_kernel, (shape((2, 1, N, N), F32), shape((2, 1, 4, N, N), BF16)),
        [ANY] + [VM] * 8 + [ANY], (ANY, ANY),
        [B16] * 6 + [pltpu.VMEM((N, NB), F32), pltpu.VMEM((8, N), F32), pltpu.VMEM((3, N, N), BF16)]
        + [pltpu.VMEM((2, N, N), F32), pltpu.SemaphoreType.DMA, pltpu.SemaphoreType.DMA((5,))],
        6, 14, {9: 1},
    )(*args)


def passed(value, down, right):
    rows, cols = lax.axis_size("row"), lax.axis_size("col")
    pairs = [
        (r * cols + c, ((r + down) % rows) * cols + (c + right) % cols)
        for r in range(rows)
        for c in range(cols)
    ]
    return lax.ppermute(value, ("row", "col"), pairs)


def on_device(diag_blocks, horizontal, vertical):
    pair = jnp.stack([horizontal[0, 0], vertical[0, 0]])
    own0, pair = lax.optimization_barrier((horizontal[0, 1], pair))
    right = passed(pair, 0, -1)
    below0 = passed(own0, -1, 1)
    state = factor_part(0, 2)(diag_blocks)
    below = passed(right, -1, 1)
    factor, e0, e1, scale0, scale1, packed = factor_part(2, 4)(*state)
    right_inverse = passed(packed, 0, -1)
    to_right, to_below, y2, y3 = products_call(horizontal, vertical, e1, scale1)
    from_left = passed(to_right, 0, 1)
    from_above = passed(to_below, 1, 0)
    below_inverse = passed(right_inverse, -1, 1)
    schur, southeast, links = local_call(
        diag_blocks, horizontal, vertical, e0, e1, scale0, scale1, y2, y3
    )
    schur0, links = right_call(horizontal, right_inverse, right, southeast, schur, links)
    schur, links = below_call(
        vertical, below_inverse, below, below0, southeast, from_left, from_above, schur0, schur, links
    )
    return (factor, schur, links)


def solution(mesh):
    blocks = P("row", "col", None, None)
    return jax.shard_map(
        on_device,
        mesh=mesh,
        in_specs=(blocks, blocks, blocks),
        out_specs=(blocks, blocks, P("row", "col", None, None, None)),
        check_vma=False,
    )
```

```python
import jax
import jax.numpy as jnp
from jax import lax
from jax.experimental import pallas as pl
from jax.experimental.pallas import tpu as pltpu
from jax.sharding import PartitionSpec as P

N = 512
NB = 128
SB = 16
F32 = jnp.float32
BF16 = jnp.bfloat16


def dot(a, b, ca=1, cb=0):
    return lax.dot_general(a, b, (((ca,), (cb,)), ((), ())), preferred_element_type=F32)


def split(x):
    hi = x.astype(BF16)
    return hi, (x - hi.astype(F32)).astype(BF16)


def dot3(a, b, cb=0):
    ah, al = a
    bh, bl = b
    if cb == 1:
        return dot(ah, bh, 1, 1) + dot(al, bh, 1, 1) + dot(ah, bl, 1, 1)
    return dot(jnp.concatenate([ah, al], 1), jnp.concatenate([bh, bh], 0)) + dot(ah, bl)


def rows8(x, k):
    return jnp.broadcast_to(x[k : k + 1, :], (8, NB))


def eliminate(s, x_ref, p_ref, s_ref):
    k0 = SB * s
    row = lax.broadcasted_iota(jnp.int32, (8, NB), 0)
    xs = [[x_ref[k0 + 8 * h : k0 + 8 * h + 8, NB * w : NB * w + NB] for h in range(2)] for w in range(2)]
    cols = [
        [jnp.broadcast_to(xs[0][h][:, k0 + c : k0 + c + 1], (8, NB)) for h in range(2)]
        for c in range(SB)
    ]
    pivots = [jnp.ones((8, NB), F32) for _ in range(2)]
    inverses = [jnp.ones((8, NB), F32) for _ in range(2)]
    saved = [[xs[w][h] for h in range(2)] for w in range(2)]
    for k in range(SB):
        kh, kr = divmod(k, 8)
        is_k = row == kr
        pivot = rows8(cols[k][kh], kr)
        inverse = 1.0 / pivot
        mult = [cols[k][h] * inverse for h in range(2)]
        mult[kh] = jnp.where(is_k, 0.0, mult[kh])
        for c in range(k + 1, SB):
            head = rows8(cols[c][kh], kr)
            cols[c] = [cols[c][h] - mult[h] * head for h in range(2)]
        pivots[kh] = jnp.where(is_k, pivot, pivots[kh])
        inverses[kh] = jnp.where(is_k, inverse, inverses[kh])
        for w in range(2):
            saved[w][kh] = jnp.where(is_k, xs[w][kh], saved[w][kh])
            head = rows8(xs[w][kh], kr)
            xs[w] = [xs[w][h] - mult[h] * head for h in range(2)]
    for h in range(2):
        scale = lax.rsqrt(pivots[h])
        s_ref[k0 + 8 * h : k0 + 8 * h + 8, 0:NB] = scale
        s_ref[k0 + 8 * h : k0 + 8 * h + 8, NB : 2 * NB] = pivots[h] * scale
        for w in range(2):
            p_ref[k0 + 8 * h : k0 + 8 * h + 8, NB * w : NB * w + NB] = saved[w][h] * scale
    below = NB - k0 - SB
    if below:
        z = jnp.concatenate(
            [jnp.concatenate([xs[w][h] * inverses[h] for w in range(2)], 1) for h in range(2)], 0
        )
        zh, zl = split(z)

        def pad(v):
            parts = [v]
            if k0:
                parts.insert(0, jnp.zeros((k0, 2 * NB), BF16))
            parts.append(jnp.zeros((below, 2 * NB), BF16))
            return jnp.concatenate(parts, 0)

        a = split(x_ref[k0 + SB : NB, 0:NB])
        x_ref[k0 + SB : NB, :] = x_ref[k0 + SB : NB, :] - dot3(a, (pad(zh), pad(zl)))


def tiled(x):
    return jnp.concatenate([x] * (N // NB), 1)


def factor_steps(first, last, g_refs, x_refs, p_refs, s_refs, w_refs, l_refs, e_refs, scale_refs):
    r_i = lax.broadcasted_iota(jnp.int32, (NB, NB), 0)
    c_i = lax.broadcasted_iota(jnp.int32, (NB, NB), 1)
    wide = lax.broadcasted_iota(jnp.int32, (NB, N), 1)
    for l_ref in l_refs:
        for c in range(first, last):
            if c:
                l_ref[0 : c * NB, (c - first) * NB : (c - first + 1) * NB] = jnp.zeros((c * NB, NB), F32)

    def outer(o, carry):
        base = pl.multiple_of(o * NB, NB)
        here = pl.ds(base, NB)
        there = pl.ds(pl.multiple_of(base - first * NB, NB), NB)
        for g_ref, x_ref in zip(g_refs, x_refs):
            x_ref[:, 0:NB] = g_ref[here, here]
            x_ref[:, NB : 2 * NB] = jnp.where(r_i == c_i, 1.0, 0.0)
        for s in range(NB // SB):
            for x_ref, p_ref, s_ref in zip(x_refs, p_refs, s_refs):
                eliminate(s, x_ref, p_ref, s_ref)
        for m in range(2):
            p_ref, s_ref, w_ref = p_refs[m], s_refs[m], w_refs[m]
            l_refs[m][here, there] = jnp.where(r_i >= c_i, p_ref[:, 0:NB].T, 0.0)
            inverse = p_ref[:, NB : 2 * NB]
            w_ref[...] = dot3(split(inverse), split(g_refs[m][here, :]))
            w_ref[:, here] = inverse
            unit = w_ref[...] * tiled(s_ref[:, NB : 2 * NB])
            e_refs[m][here, :] = jnp.where(wide < base + NB, unit, 0.0).astype(BF16)
            scale_refs[m][here, :] = s_ref[:, 0:NB]
        for p in range(first + 1, N // NB):
            rows = slice(p * NB, (p + 1) * NB)

            @pl.when(p > o)
            def _():
                for g_ref, p_ref, w_ref, l_ref in zip(g_refs, p_refs, w_refs, l_refs):
                    lower = dot3(split(g_ref[rows, here]), split(p_ref[:, NB : 2 * NB]), 1)
                    l_ref[rows, there] = lower
                    g_ref[rows, here] = jnp.zeros((NB, NB), F32)
                    g_ref[rows, :] = g_ref[rows, :] - dot3(split(lower), split(w_ref[...]))

        return carry

    lax.fori_loop(first, last, outer, 0)


LOWER = [(r, c) for r in range(N // NB) for c in range(r)]
TAIL = 8 * NB
PACKED = TAIL + SB


def block(ref, r, c):
    return ref[r * NB : (r + 1) * NB, c * NB : (c + 1) * NB]


def at(first, b):
    return slice(first + b * NB, first + (b + 1) * NB)


def iotas():
    return (
        lax.broadcasted_iota(jnp.int32, (NB, NB), 0),
        lax.broadcasted_iota(jnp.int32, (NB, NB), 1),
    )


def pick_rows(rows):
    where = lax.broadcasted_iota(jnp.int32, (SB, NB), 0)
    tile = jnp.zeros((SB, NB), F32)
    for k, row in enumerate(rows):
        tile = jnp.where(where == k, jnp.broadcast_to(row, (SB, NB)), tile)
    return tile


def pack_unit(e_ref, scale_ref, dst_ref):
    r_i, c_i = iotas()
    for b, (r, c) in enumerate(LOWER):
        dst_ref[at(0, b), :] = block(e_ref, r, c)
    for k in range(2):
        one = block(e_ref, 2 * k, 2 * k).astype(F32)
        two = block(e_ref, 2 * k + 1, 2 * k + 1).astype(F32).T
        dst_ref[at(0, 6 + k), :] = jnp.where(r_i > c_i, one, jnp.where(r_i < c_i, two, 0.0)).astype(BF16)
    parts = [[], [], []]
    for k in range(N // NB):
        rest = scale_ref[k * NB : (k + 1) * NB, :].T[0:1, :]
        for part in parts:
            part.append(rest)
            rest = rest - rest.astype(BF16).astype(F32)
    dst_ref[TAIL:PACKED, :] = pick_rows(sum(parts, [])).astype(BF16)


def unpack_unit(src_ref, e_ref, scale_ref, row_ref):
    r_i, c_i = iotas()
    eye = jnp.where(r_i == c_i, 1.0, 0.0)
    zero = jnp.zeros((NB, NB), BF16)
    for b, (r, c) in enumerate(LOWER):
        e_ref[r * NB : (r + 1) * NB, c * NB : (c + 1) * NB] = src_ref[at(0, b), :]
        e_ref[c * NB : (c + 1) * NB, r * NB : (r + 1) * NB] = zero
    for k in range(2):
        pair = src_ref[at(0, 6 + k), :].astype(F32)
        for d, value in ((2 * k, pair), (2 * k + 1, pair.T)):
            e_ref[d * NB : (d + 1) * NB, d * NB : (d + 1) * NB] = jnp.where(r_i > c_i, value, eye).astype(BF16)
    tile = src_ref[TAIL:PACKED, :].astype(F32)
    for k in range(N // NB):
        row = tile[k : k + 1, :] + tile[4 + k : 5 + k, :] + tile[8 + k : 9 + k, :]
        row_ref[:, k * NB : (k + 1) * NB] = jnp.broadcast_to(row, (8, NB))
        scale_ref[k * NB : (k + 1) * NB, :] = jnp.broadcast_to(row, (NB, NB)).T


def scale_row(scale_ref, row_ref):
    for k in range(N // NB):
        row_ref[:, k * NB : (k + 1) * NB] = scale_ref[k * NB : (k + 1) * NB, :].T[0:8, :]


def pack_symmetric(value, dst_ref):
    r_i, c_i = iotas()
    for b, (r, c) in enumerate(LOWER):
        dst_ref[at(0, b), :] = block(value, r, c).astype(BF16)
    rows = []
    for k in range(2):
        two = block(value, 2 * k + 1, 2 * k + 1)
        dst_ref[at(0, 6 + k), :] = jnp.where(r_i >= c_i, block(value, 2 * k, 2 * k), two).astype(BF16)
        rows.append(jnp.sum(jnp.where(r_i == c_i, two, 0.0), 0, keepdims=True))
    dst_ref[TAIL:PACKED, :] = pick_rows(rows).astype(BF16)


def add_symmetric(src_ref, dst_ref):
    r_i, c_i = iotas()

    def sub(r, c, value):
        rows, cols = slice(r * NB, (r + 1) * NB), slice(c * NB, (c + 1) * NB)
        dst_ref[rows, cols] = dst_ref[rows, cols] - value

    for b, (r, c) in enumerate(LOWER):
        value = src_ref[at(0, b), :].astype(F32)
        sub(r, c, value)
        sub(c, r, value.T)
    tile = src_ref[TAIL:PACKED, :].astype(F32)
    for k in range(2):
        pair = src_ref[at(0, 6 + k), :].astype(F32)
        turned = pair.T
        sub(2 * k, 2 * k, jnp.where(r_i >= c_i, pair, turned))
        diagonal = jnp.broadcast_to(tile[k : k + 1, :], (NB, NB))
        two = jnp.where(r_i < c_i, pair, turned)
        sub(2 * k + 1, 2 * k + 1, jnp.where(r_i == c_i, diagonal, two))


def solve_t(e_ref, row_ref, c_ref, out_ref):
    h = N // 2
    row = row_ref[0:1, :]
    out_ref[:, 0:h] = (dot(c_ref[:, 0:h], e_ref[0:h, 0:h], 1, 1) * row[:, 0:h]).astype(BF16)
    out_ref[:, h:N] = (dot(c_ref[...], e_ref[h:N, :], 1, 1) * row[:, h:N]).astype(BF16)


def solve_n(e_ref, scale_ref, c_ref, out_ref):
    h = N // 2
    out_ref[0:h, :] = (dot(e_ref[0:h, 0:h], c_ref[0:h, :]) * tiled(scale_ref[0:h, :])).astype(BF16)
    out_ref[h:N, :] = (dot(e_ref[h:N, :], c_ref[...]) * tiled(scale_ref[h:N, :])).astype(BF16)


ANY = pl.BlockSpec(memory_space=pl.ANY)
VM = pl.BlockSpec(memory_space=pltpu.VMEM)
B16 = pltpu.VMEM((N, N), BF16)
WIDE = pltpu.VMEM((N, N), F32)


def shape(dims, kind):
    return jax.ShapeDtypeStruct(dims, kind)


def call(kernel, outs, in_specs, out_specs, scratch, flops, limit, aliases=None):
    return pl.pallas_call(
        kernel,
        out_shape=outs,
        in_specs=in_specs,
        out_specs=out_specs,
        scratch_shapes=scratch,
        input_output_aliases=aliases or {},
        compiler_params=pltpu.CompilerParams(vmem_limit_bytes=limit << 20),
        cost_estimate=pl.CostEstimate(flops=flops * 10**9, bytes_accessed=4 << 20, transcendentals=0),
    )


WORK = [pltpu.VMEM((NB, 2 * NB), F32)] * 6 + [pltpu.VMEM((NB, N), F32)] * 2 + [WIDE] * 2
DMA2 = pltpu.SemaphoreType.DMA((2,))
ENDS = (shape((N, N), BF16), shape((N, N), BF16), shape((N, NB), F32), shape((N, NB), F32))


def factor_part(first, last):
    lo, hi = first * NB, last * NB
    ending = hi == N

    def kernel(*refs):
        refs = list(refs)
        take = lambda n: [refs.pop(0) for _ in range(n)]
        source = None if first else take(1)[0]
        before = take(6) if first else ()
        l0, l1 = take(2)
        after = take(5) if ending else take(6)
        x0, x1, p0, p1, s0, s1, w0, w1, g0, g1 = take(10)
        state = tuple(after[:4]) if ending else tuple(take(4))
        in_sem = take(1)[0]
        if first:
            for dst, src in zip((g0, g1), before):
                dst[lo:N, :] = src[...]
            for dst, src in zip(state, before[2:]):
                dst[0:lo, :] = src[...]
        else:
            copies = [
                pltpu.make_async_copy(source.at[m, m], g_ref, in_sem.at[m])
                for m, g_ref in enumerate((g0, g1))
            ]
            for c in copies:
                c.start()
            for c in copies:
                c.wait()
        factor_steps(first, last, (g0, g1), (x0, x1), (p0, p1), (s0, s1), (w0, w1), (l0, l1), state[:2], state[2:])
        if ending:
            pack_unit(state[0], state[2], after[4])
        else:
            for dst, src in zip(after, (g0, g1)):
                dst[...] = src[hi:N, :]
            for dst, src in zip(after[2:], state):
                dst[...] = src[0:hi, :]

    if ending:
        outs = ENDS + (shape((PACKED, NB), BF16),)
        scratch = []
    else:
        outs = (shape((N - hi, N), F32),) * 2 + (shape((hi, N), BF16),) * 2 + (shape((hi, NB), F32),) * 2
        scratch = [B16, B16, pltpu.VMEM((N, NB), F32), pltpu.VMEM((N, NB), F32)]
    return call(
        kernel, (shape((N, hi - lo), F32),) * 2 + outs,
        [VM] * 6 if first else [ANY], (VM,) * (2 + len(outs)),
        WORK + scratch + [DMA2], 15 * (last - first), 13,
    )


def products_kernel(h_ref, v_ref, e1, scale1, to_right, to_below, y2, y3, c2, c3, in_sem):
    copies = [
        pltpu.make_async_copy(h_ref.at[1, 1], c2, in_sem.at[0]),
        pltpu.make_async_copy(v_ref.at[1, 1], c3, in_sem.at[1]),
    ]
    for c in copies:
        c.start()
    for c in copies:
        c.wait()
    solve_n(e1, scale1, c2, y2)
    solve_n(e1, scale1, c3, y3)
    t2 = y2[...].T
    pack_symmetric(dot(t2, y2[...]), to_right)
    side = dot(t2, y3[...])
    for r in range(N // NB):
        for c in range(N // NB):
            to_right[at(PACKED, 4 * r + c), :] = block(side, r, c).astype(BF16)
    pack_symmetric(dot(y3[...].T, y3[...]), to_below)


def products_call(*args):
    return call(
        products_kernel,
        (shape((PACKED + N * N // NB, NB), BF16), shape((PACKED, NB), BF16), shape((N, N), BF16),
         shape((N, N), BF16)),
        [ANY] * 2 + [VM] * 2, (VM,) * 4, [B16, B16, DMA2], 4, 8,
    )(*args)


def local_kernel(d_ref, h_ref, v_ref, e0, e1, scale0, scale1, y2, y3, la0, la1, lb0, lb1,
                 l_out, sbuf, dbuf, link_out,
                 c0, c1, f2, f3, y0, y1, z2, z3, lbuf, row1, in_sem, out_sem, l_sem):
    copies = [
        pltpu.make_async_copy(src, dst, in_sem.at[k])
        for k, (src, dst) in enumerate(
            (
                (h_ref.at[1, 0], c0),
                (v_ref.at[0, 1], c1),
                (h_ref.at[0, 0], f2),
                (v_ref.at[0, 0], f3),
                (d_ref.at[0, 1], sbuf.at[0]),
                (d_ref.at[1, 0], sbuf.at[1]),
            )
        )
    ]
    for c in copies:
        c.start()
    half = N // 2
    factors = [
        pltpu.make_async_copy(src, l_out.at[k % 2, 0, :, k // 2 * half : (k // 2 + 1) * half], l_sem.at[k])
        for k, src in enumerate((la0, la1, lb0, lb1))
    ]
    for c in factors:
        c.start()
    scale_row(scale1, row1)
    for c in copies[:4]:
        c.wait()
    outs = []
    solve_t(e1, row1, c1, y1)
    put_link(outs, lbuf, link_out, out_sem, 0, 1, dot(y1[...], y3[...]))
    solve_t(e1, row1, c0, y0)
    put_link(outs, lbuf, link_out, out_sem, 1, 0, dot(y0[...], y2[...]))
    solve_n(e0, scale0, f2, z2)
    solve_n(e0, scale0, f3, z3)
    u2 = z2[...].T
    put_link(outs, lbuf, link_out, out_sem, 0, 3, dot(u2, z3[...]) + dot(y1[...], y0[...], 1, 1))
    dbuf[0] = dot(y1[...], y2[...])
    dbuf[1] = dot(y0[...], y3[...])
    for c in copies[4:]:
        c.wait()
    sbuf[0] = sbuf[0] - (dot(u2, z2[...]) + dot(y1[...], y1[...], 1, 1))
    sbuf[1] = sbuf[1] - (dot(z3[...].T, z3[...]) + dot(y0[...], y0[...], 1, 1))
    for c in outs + factors:
        c.wait()


def local_call(*args):
    return call(
        local_kernel,
        (shape((2, 1, N, N), F32), shape((2, N, N), F32), shape((2, N, N), F32), shape((2, 1, 4, N, N), BF16)),
        [ANY] * 3 + [VM] * 10, (ANY, VM, VM, ANY),
        [B16] * 8 + [pltpu.VMEM((3, N, N), BF16), pltpu.VMEM((8, N), F32)]
        + [pltpu.SemaphoreType.DMA((6,)), pltpu.SemaphoreType.DMA((3,)), pltpu.SemaphoreType.DMA((4,))],
        9, 16,
    )(*args)


def put_link(outs, buffer, out, sem, row, which, value):
    slot = len(outs)
    buffer[slot] = (-value).astype(BF16)
    copy = pltpu.make_async_copy(buffer.at[slot], out.at[row, 0, which], sem.at[slot])
    copy.start()
    outs.append(copy)


def right_kernel(h_ref, rpack, rc, se, schur_in, link_in, schur0, link_out,
                 inv, c0, w0, w2, w3, scale, row, lbuf, in_sem, sem):
    load = pltpu.make_async_copy(h_ref.at[0, 1], c0, in_sem)
    load.start()
    unpack_unit(rpack, inv, scale, row)
    load.wait()
    outs = []
    solve_t(inv, row, c0, w0)
    solve_n(inv, scale, rc.at[0], w2)
    put_link(outs, lbuf, link_out, sem, 0, 0, dot(w0[...], w2[...]))
    solve_n(inv, scale, rc.at[1], w3)
    put_link(outs, lbuf, link_out, sem, 0, 2, dot(w0[...], w3[...]) + se[0])
    schur0[...] = schur_in[0] - dot(w0[...], w0[...], 1, 1)
    for c in outs:
        c.wait()


def right_call(*args):
    return call(
        right_kernel, (shape((N, N), F32), shape((2, 1, 4, N, N), BF16)),
        [ANY] + [VM] * 4 + [ANY], (VM, ANY),
        [B16] * 5 + [pltpu.VMEM((N, NB), F32), pltpu.VMEM((8, N), F32), pltpu.VMEM((2, N, N), BF16)]
        + [pltpu.SemaphoreType.DMA, DMA2],
        5, 10, {5: 1},
    )(*args)


def below_kernel(v_ref, bpack, bc, bc0, se, from_left, from_above, schur0, schur_in, link_in, schur_out, link_out,
                 inv, c1, w0, w1, w2, w3, scale, row, lbuf, sbuf, in_sem, sem):
    load = pltpu.make_async_copy(v_ref.at[1, 0], c1, in_sem)
    load.start()
    unpack_unit(bpack, inv, scale, row)
    sbuf[0] = schur0[...]
    add_symmetric(from_above, sbuf.at[0])
    stores = [pltpu.make_async_copy(sbuf.at[m], schur_out.at[m, 0], sem.at[3 + m]) for m in range(2)]
    stores[0].start()
    load.wait()
    outs = []
    solve_t(inv, row, c1, w1)
    sbuf[1] = schur_in[1] - dot(w1[...], w1[...], 1, 1)
    add_symmetric(from_left, sbuf.at[1])
    stores[1].start()
    solve_n(inv, scale, bc.at[1], w3)
    put_link(outs, lbuf, link_out, sem, 1, 1, dot(w1[...], w3[...]))
    solve_n(inv, scale, bc.at[0], w2)
    put_link(outs, lbuf, link_out, sem, 1, 2, dot(w1[...], w2[...]) + se[1])
    solve_t(inv, row, bc0, w0)
    side = jnp.concatenate(
        [
            jnp.concatenate([from_left[at(PACKED, 4 * r + c), :] for c in range(N // NB)], 1)
            for r in range(N // NB)
        ],
        0,
    )
    put_link(outs, lbuf, link_out, sem, 1, 3, dot(w1[...], w0[...], 1, 1) + side.astype(F32))
    for c in outs + stores:
        c.wait()


def below_call(*args):
    return call(
        below_kernel, (shape((2, 1, N, N), F32), shape((2, 1, 4, N, N), BF16)),
        [ANY] + [VM] * 8 + [ANY], (ANY, ANY),
        [B16] * 6 + [pltpu.VMEM((N, NB), F32), pltpu.VMEM((8, N), F32), pltpu.VMEM((3, N, N), BF16)]
        + [pltpu.VMEM((2, N, N), F32), pltpu.SemaphoreType.DMA, pltpu.SemaphoreType.DMA((5,))],
        6, 14, {9: 1},
    )(*args)


def passed(value, down, right):
    rows, cols = lax.axis_size("row"), lax.axis_size("col")
    pairs = [
        (r * cols + c, ((r + down) % rows) * cols + (c + right) % cols)
        for r in range(rows)
        for c in range(cols)
    ]
    return lax.ppermute(value, ("row", "col"), pairs)


def on_device(diag_blocks, horizontal, vertical):
    pair = jnp.stack([horizontal[0, 0], vertical[0, 0]])
    own0, pair = lax.optimization_barrier((horizontal[0, 1], pair))
    right = passed(pair, 0, -1)
    below0 = passed(own0, -1, 1)
    la0, la1, *state = factor_part(0, 2)(diag_blocks)
    below = passed(right, -1, 1)
    lb0, lb1, e0, e1, scale0, scale1, packed = factor_part(2, 4)(*state)
    right_inverse = passed(packed, 0, -1)
    to_right, to_below, y2, y3 = products_call(horizontal, vertical, e1, scale1)
    from_left = passed(to_right, 0, 1)
    from_above = passed(to_below, 1, 0)
    below_inverse = passed(right_inverse, -1, 1)
    factor, schur, southeast, links = local_call(
        diag_blocks, horizontal, vertical, e0, e1, scale0, scale1, y2, y3, la0, la1, lb0, lb1
    )
    schur0, links = right_call(horizontal, right_inverse, right, southeast, schur, links)
    schur, links = below_call(
        vertical, below_inverse, below, below0, southeast, from_left, from_above, schur0, schur, links
    )
    return (factor, schur, links)


def solution(mesh):
    blocks = P("row", "col", None, None)
    return jax.shard_map(
        on_device,
        mesh=mesh,
        in_specs=(blocks, blocks, blocks),
        out_specs=(blocks, blocks, P("row", "col", None, None, None)),
        check_vma=False,
    )
```
